32 devices in a mesh: seq: 8 (over z, y), head: 4 (over x, core).
Axes of the slice: x: 2, y: 2, z: 4, core: 2. Of those that a mesh axis runs over, the one named last changes fastest.
Arguments:
- layer_in: bfloat16 [4096, 2048], P('seq', 'head'), may hold values from -6 to 6
- query_weight: bfloat16 [2048, 1024], P(None, 'head'), may hold values from -0.125 to 0.125
- key_weight: bfloat16 [2048, 1024], P(None, 'head'), may hold values from -0.125 to 0.125
- value_weight: bfloat16 [2048, 1024], P(None, 'head'), may hold values from -0.125 to 0.125
- gate_weight: bfloat16 [2048, 1024], P(None, 'head'), may hold values from -0.125 to 0.125
- beta_weight: bfloat16 [2048, 8], P(None, 'head'), may hold values from -0.125 to 0.125
- decay_weight: bfloat16 [2048, 8], P(None, 'head'), may hold values from -0.125 to 0.125
- conv_weight: float32 [4, 3, 1024], P(None, None, 'head'), may hold values from -3 to 3
- decay_log: float32 [8], P('head'), as said below
- beta_bias: float32 [8], P('head'), as said below
- decay_bias: float32 [8], P('head'), may hold values from -1 to 1
- norm_gain: float32 [128], replicated, may hold values from 0.1 to 1.9
- out_weight: bfloat16 [1024, 2048], P('head'), may hold values from -0.1875 to 0.1875
Outputs:
- layer_out: bfloat16 [4096, 2048], P('seq', 'head')
The draws below stay inside these ranges and needn't reach their ends.
Inputs may be any that keep to these rules, and one draw needn't show every extreme that they name: decay_log lies between log(0.1 / 4096) and log(0.05). beta_bias lies between log(0.5 * 128 / 4096) and 1.
All inputs are finite; a program needn't handle non-finite values.
Results may differ from the reference program's by a relative error of at most 0.0049.
Values may be sent and summed in bfloat16 or wider, within the bound.
A program may use at most 128 MiB of HBM per device.

```python
import jax
import jax.numpy as jnp
from jax import lax

D = 2048
HEADS = 8
HDIM = 128
CONV = 4
BLOCK = 128
TOKENS = 4096


def head_kinds(key):
    pair_count = HEADS // 2
    pick_one = jax.random.randint(jax.random.fold_in(key, 31), (pair_count,), 0, 2)
    rolled = jax.random.randint(jax.random.fold_in(key, 32), (pair_count,), 0, 100)
    limit = 25
    both_slow = rolled < limit
    first_slow = (pick_one == 0) | both_slow
    second_slow = (pick_one == 1) | both_slow
    return jnp.stack([first_slow, second_slow], axis=1).reshape(HEADS)


def draw_decay_log(key, part):
    slow_heads = head_kinds(key)
    spread = jax.random.uniform(jax.random.fold_in(key, 41), (HEADS,), jnp.float32)
    slow_rate = jnp.log((0.1 + 0.4 * spread) / TOKENS)
    fast_rate = jnp.log(0.02 + 0.03 * spread)
    return jnp.where(slow_heads, slow_rate, fast_rate).astype(jnp.float32)


def draw_beta_bias(key, part):
    slow_heads = head_kinds(key)
    spread = jax.random.uniform(jax.random.fold_in(key, 42), (HEADS,), jnp.float32)
    slow_bias = jnp.log((0.5 + 0.5 * spread) * HDIM / TOKENS)
    fast_bias = 2.0 * spread - 1.0
    return jnp.where(slow_heads, slow_bias, fast_bias).astype(jnp.float32)


def shard_levels(rng, shape, shards, smallest, high):
    loudness = 1.0
    for position, shards_of in shards:
        steps = jax.random.uniform(jax.random.fold_in(jax.random.fold_in(rng, 6), position), (shards_of,), jnp.float32, smallest / len(shards), high / len(shards))
        loudness = loudness * jnp.repeat(jnp.exp(steps), shape[position] // shards_of).reshape((-1,) + (1,) * (len(shape) - 1 - position))
    return loudness


def bell_draw(rng, extent, width, reach, pieces=(), kind=jnp.bfloat16):
    values = width * jax.random.normal(rng, extent, jnp.float32)
    if pieces:
        values = values * shard_levels(rng, extent, pieces, -0.22, 0.18)
    return jnp.clip(values, -reach, reach).astype(kind)


def setup_inputs(seed: int = 0) -> dict:
    seeds = jax.random.split(jax.random.key(seed), 14)
    layer_in = bell_draw(seeds[0], (TOKENS, D), 1.0, 6.0, ((0, 8), (1, 4)))
    query_weight = bell_draw(seeds[1], (D, HEADS * HDIM), D ** -0.5, 0.125, ((1, 4),))
    key_weight = bell_draw(seeds[2], (D, HEADS * HDIM), D ** -0.5, 0.125, ((1, 4),))
    value_weight = bell_draw(seeds[3], (D, HEADS * HDIM), D ** -0.5, 0.125, ((1, 4),))
    gate_weight = bell_draw(seeds[4], (D, HEADS * HDIM), D ** -0.5, 0.125, ((1, 4),))
    beta_weight = bell_draw(seeds[5], (D, HEADS), D ** -0.5, 0.125, ((1, 4),))
    decay_weight = bell_draw(seeds[6], (D, HEADS), D ** -0.5, 0.125, ((1, 4),))
    conv_weight = bell_draw(seeds[7], (CONV, 3, HEADS * HDIM), 0.5, 3.0, ((2, 4),), jnp.float32)
    decay_log = draw_decay_log(jax.random.fold_in(seeds[13], 71), 0)
    beta_bias = draw_beta_bias(jax.random.fold_in(seeds[13], 71), 0)
    decay_bias = jnp.clip(jax.random.uniform(seeds[10], (HEADS,), jnp.float32, -1.0, 1.0) * shard_levels(seeds[10], (HEADS,), ((0, 4),), -0.4, 0.0), -1.0, 1.0)
    norm_gain = jnp.clip(1.0 + 0.18 * jax.random.normal(seeds[11], (HDIM,), jnp.float32), 0.1, 1.9)
    out_weight = bell_draw(seeds[12], (HEADS * HDIM, D), (HEADS * HDIM) ** -0.5, 0.1875, ((0, 4),))
    return {"layer_in": layer_in, "query_weight": query_weight, "key_weight": key_weight, "value_weight": value_weight, "gate_weight": gate_weight, "beta_weight": beta_weight, "decay_weight": decay_weight, "conv_weight": conv_weight, "decay_log": decay_log, "beta_bias": beta_bias, "decay_bias": decay_bias, "norm_gain": norm_gain, "out_weight": out_weight}


exact_mode = lax.Precision.HIGHEST
norm_floor = 0.0001

def causal_conv(values, kernel):
    taps = kernel.shape[0]
    summed = kernel[0] * values
    for offset in range(1, taps):
        shifted = jnp.concatenate([jnp.zeros((offset, values.shape[1]), jnp.float32), values[:-offset]], axis=0)
        summed = summed + kernel[offset] * shifted
    return jax.nn.silu(summed)

def unit_rows(values):
    return values * lax.rsqrt(lax.optimization_barrier(jnp.sum(values * values, axis=-1, keepdims=True)) + 1.0)

def block_terms(queries, key_rows, values, beta_gate, log_decay):
    length = log_decay.shape[-1]
    running = jnp.cumsum(log_decay, axis=-1)
    row_index = lax.broadcasted_iota(jnp.int32, (length, length), 0)
    col_index = lax.broadcasted_iota(jnp.int32, (length, length), 1)
    within = row_index >= col_index
    before = row_index > col_index
    spread = running[..., :, None] - running[..., None, :]
    decay_matrix = jnp.where(within, jnp.exp(jnp.minimum(spread, 0.0)), 0.0)
    key_gram = jnp.einsum('...rd,...sd->...rs', key_rows, key_rows, precision=exact_mode)
    lower_part = jnp.where(before, beta_gate[..., :, None] * decay_matrix * key_gram, 0.0)
    system = lower_part + jnp.eye(length, dtype=jnp.float32)
    growth = jnp.exp(running)
    right_side = jnp.concatenate([beta_gate[..., None] * values, (beta_gate * growth)[..., None] * key_rows], axis=-1)
    solved = lax.linalg.triangular_solve(system, right_side, left_side=True, lower=True, unit_diagonal=True)
    value_dim = values.shape[-1]
    fixed_rows = solved[..., :value_dim]
    erased = solved[..., value_dim:]
    query_key = jnp.einsum('...rd,...sd->...rs', queries, key_rows, precision=exact_mode)
    mixing = jnp.where(within, decay_matrix * query_key, 0.0)
    local_out = jnp.einsum('...rs,...se->...re', mixing, fixed_rows, precision=exact_mode)
    reader = growth[..., None] * queries - jnp.einsum('...rs,...sd->...rd', mixing, erased, precision=exact_mode)
    tail_decay = jnp.exp(running[..., -1:] - running)
    weighted = tail_decay[..., None] * key_rows
    key_dim = key_rows.shape[-1]
    transit = jnp.exp(running[..., -1])[..., None, None] * jnp.eye(key_dim, dtype=jnp.float32) - jnp.einsum('...bd,...be->...de', weighted, erased, precision=exact_mode)
    carried = jnp.einsum('...bd,...be->...de', weighted, fixed_rows, precision=exact_mode)
    return (local_out, reader, transit, carried)

def reference(layer_in, query_weight, key_weight, value_weight, gate_weight, beta_weight, decay_weight, conv_weight, decay_log, beta_bias, decay_bias, norm_gain, out_weight):
    tokens = layer_in.shape[0]

    def project(weight):
        return jnp.dot(layer_in.astype(jnp.float32), weight.astype(jnp.float32), preferred_element_type=jnp.float32)
    mixed_query = causal_conv(project(query_weight), conv_weight[:, 0])
    mixed_key = causal_conv(project(key_weight), conv_weight[:, 1])
    mixed_value = causal_conv(project(value_weight), conv_weight[:, 2])
    queries = unit_rows(mixed_query.reshape(tokens, HEADS, HDIM))
    key_rows = unit_rows(mixed_key.reshape(tokens, HEADS, HDIM))
    values = mixed_value.reshape(tokens, HEADS, HDIM)
    beta_gate = jax.nn.sigmoid(project(beta_weight) + beta_bias)
    log_decay = -jnp.exp(decay_log) * jax.nn.softplus(project(decay_weight) + decay_bias)
    blocks = tokens // BLOCK

    def arrange(array):
        return array.reshape(blocks, BLOCK, HEADS, HDIM).transpose(0, 2, 1, 3)

    def arrange_gate(array):
        return array.reshape(blocks, BLOCK, HEADS).transpose(0, 2, 1)

    def advance(carry_state, inputs):
        local_out, reader, transit, carried = block_terms(*inputs)
        output = local_out + jnp.einsum('hrd,hde->hre', reader, carry_state, precision=exact_mode)
        carry_state = jnp.einsum('hde,hef->hdf', transit, carry_state, precision=exact_mode) + carried
        return (carry_state, output)
    zero_state = jnp.zeros((HEADS, HDIM, HDIM), jnp.float32)
    last_state, outputs = lax.scan(advance, zero_state, (arrange(queries), arrange(key_rows), arrange(values), arrange_gate(beta_gate), arrange_gate(log_decay)))
    head_out = outputs.transpose(0, 2, 1, 3).reshape(tokens, HEADS, HDIM)
    gate_rows = project(gate_weight).reshape(tokens, HEADS, HDIM)
    scaled = head_out * lax.rsqrt(lax.optimization_barrier(jnp.mean(head_out * head_out, axis=-1, keepdims=True)) + norm_floor)
    hidden = (scaled * norm_gain * jax.nn.silu(gate_rows)).reshape(tokens, HEADS * HDIM).astype(jnp.bfloat16)
    return jnp.dot(hidden.astype(jnp.float32), out_weight.astype(jnp.float32), preferred_element_type=jnp.float32).astype(jnp.bfloat16)
```

```python
import functools

import jax
import jax.numpy as jnp
from jax import lax
from jax.experimental import pallas as pl
from jax.experimental.pallas import tpu as pltpu
from jax.sharding import PartitionSpec as P

BLOCK = 128
PRIOR = 8
LANES = 128
PIECE = 64
BASE = 8
MESH = pl.DeviceIdType.MESH
F32 = jnp.float32
BF16 = jnp.bfloat16
norm_floor = 0.0001


def bits_below(limit):
    found = []
    bit = limit // 2
    while bit:
        found.append(bit)
        bit //= 2
    return found


def low_bit(value):
    return value & -value


def rounds_of(seqs):
    found = []
    half = 2
    while half < seqs:
        found.append(half)
        half *= 2
    return found


def meet(peers):
    barrier = pltpu.get_barrier_semaphore()
    expected = 0
    for present, device in peers:
        if present is True:
            pl.semaphore_signal(barrier, inc=1, device_id=device, device_id_type=MESH)
            expected = expected + 1
        else:

            @pl.when(present)
            def _():
                pl.semaphore_signal(barrier, inc=1, device_id=device, device_id_type=MESH)

            expected = expected + present.astype(jnp.int32)
    pl.semaphore_wait(barrier, expected)


def remote(source, target, send_sem, recv_sem, device):
    return pltpu.make_async_remote_copy(
        src_ref=source,
        dst_ref=target,
        send_sem=send_sem,
        recv_sem=recv_sem,
        device_id=device,
        device_id_type=MESH,
    )


def dot(left, right, contract=((1,), (0,))):
    return lax.dot_general(
        left.astype(BF16), right.astype(BF16), (contract, ((), ())), preferred_element_type=F32
    )


def split(value):
    high = value.astype(BF16)
    return high, (value - high.astype(F32)).astype(BF16)


def dot3(left, right, contract=((1,), (0,))):
    lh, ll = left if isinstance(left, tuple) else split(left)
    rh, rl = right if isinstance(right, tuple) else split(right)
    axis = contract[1][0]
    both = dot(jnp.concatenate([lh, lh], axis=1), jnp.concatenate([rh, rl], axis=axis), contract)
    return both + dot(ll, rh, contract)


def layer_kernel(
    seqs, n, heads,
    x_ref, wq, wk, wv, wg, beta_in, step_in, taps_in, rates_in, bias_in, shift_in, gain_in, w_ref,
    out_ref,
    w_all, w_flat, spread, x_own, buf, prior, raw, local, reader,
    slab_a, slab_c, mate_a, mate_c, go_a, go_c, in_a, in_c, pre_a, pre_c,
    w_buf, hid,
    beta_ref, step_ref, taps, gain, rates, beta_bias, decay_bias,
    load_sem, small_sem, x_sem, x_send, x_recv, p_send, p_recv, own_sem, w_send, w_recv,
    v_send, v_recv, sa_send, sa_recv, sc_send, sc_recv, side_send, a_send, a_recv, c_send, c_recv,
    h_send, h_recv,
):
    seq = lax.axis_index("seq")
    me = lax.axis_index("head")
    tokens, feats = x_ref.shape
    width = wq.shape[1]
    dim = LANES
    blocks = tokens // BLOCK
    columns = out_ref.shape[1]
    pieces = tokens // PIECE
    per_block = BLOCK // PIECE
    main = 2 * width + LANES
    total_width = w_all.shape[1]
    q_at = main
    g_at = main + width
    bits = bits_below(n)

    own_load = pltpu.make_async_copy(x_ref, x_own, x_sem)
    own_load.start()
    loads = []
    for i, (w, at) in enumerate(((wk, 0), (wv, width), (wq, q_at), (wg, g_at))):
        loads.append(pltpu.make_async_copy(w, w_all.at[:, pl.ds(at, width)], load_sem.at[i]))
    smalls = [
        pltpu.make_async_copy(source, target, small_sem.at[i])
        for i, (source, target) in enumerate((
            (beta_in, beta_ref), (step_in, step_ref), (taps_in, taps), (gain_in, gain),
            (rates_in, rates), (bias_in, beta_bias), (shift_in, decay_bias),
        ))
    ]
    for load in smalls + loads:
        load.start()
    has_next = seq < seqs - 1
    has_before = seq > 0
    odd = seq % 2
    is_odd = odd == 1
    mate = seq + 1 - 2 * odd
    lone = heads // 2
    rounds = rounds_of(seqs)
    uppers, sources, origins, whole = [], [], [], []
    for half in rounds:
        inside = seq % (2 * half)
        uppers.append(inside >= half)
        sources.append(inside // 2 == half // 2 - 1)
        origins.append(seq - inside + half - 2 + odd)
        whole.append(seq - inside > 0)
    starts = seq == 1 if rounds else seq < 0
    gives_c = [seq >= 0 if h < lone else seq != 1 for h in range(heads)]
    gives_a = [seq != 0 if h < lone else seq >= 2 for h in range(heads)]
    takes_c = [seq >= 0 if h < lone else seq != 0 for h in range(heads)]
    takes_a = [seq != 1 if h < lone else seq >= 2 for h in range(heads)]
    peers = [(True, (seq, me ^ m)) for m in range(1, n)]
    peers += [(has_next, (seq + 1, me ^ m)) for m in range(n)]
    peers += [(has_before, (seq - 1, me ^ m)) for m in range(n)]
    for r, half in enumerate(rounds):
        peers += [(sources[r], (seq + 2 + 2 * j, me)) for j in range(half // 2)]
        peers += [(uppers[r], (origins[r], me))]
    meet(peers)
    own_load.wait()

    def hop(m, bit, c):
        piece = pl.ds(c * PIECE, PIECE)
        source = x_own.at[piece] if m == 0 else buf.at[m, piece]
        got = m | bit
        return remote(
            source, buf.at[got, piece], x_send.at[got, c], x_recv.at[got, c], (seq, me ^ bit)
        )

    tails = [
        remote(
            x_own.at[pl.ds(tokens - PRIOR, PRIOR)],
            prior.at[m],
            p_send.at[m],
            p_recv.at[m],
            (seq + 1, me ^ m),
        )
        for m in range(n)
    ]

    @pl.when(has_next)
    def _():
        for tail in tails:
            tail.start()

    hops = {}
    for c in range(pieces):
        for bit in bits:
            hops[bit, c] = hop(0, bit, c)
            hops[bit, c].start()

    row = lax.broadcasted_iota(jnp.int32, (BLOCK, BLOCK), 0)
    col = lax.broadcasted_iota(jnp.int32, (BLOCK, BLOCK), 1)
    for j in range(BASE - 1):
        spread[:, pl.ds(j * LANES, LANES)] = (row == col // BASE * BASE + j).astype(F32).astype(BF16)

    for load in smalls:
        load.wait()
    w_flat[...] = jnp.zeros(w_flat.shape, F32)
    w_flat[pl.ds(0, heads), :] = beta_ref[...].astype(F32)
    w_flat[pl.ds(heads, heads), :] = step_ref[...].astype(F32)
    for i in range(w_flat.shape[1] // LANES):
        piece = pl.ds(i * LANES, LANES)
        w_all[piece, pl.ds(2 * width, LANES)] = w_flat[:, piece].T.astype(BF16)
    for load in loads:
        load.wait()

    def weights_of(m, cols):
        start = pl.multiple_of((me ^ m) * feats, LANES)
        return w_all[pl.ds(start, feats), cols]

    def arrive(m, c):
        hops[m, c].wait_recv()
        for bit in bits:
            if bit < low_bit(m):
                hops[m | bit, c] = hop(m, bit, c)
                hops[m | bit, c].start()

    every = pl.ds(0, total_width)
    first_cols = pl.ds(0, main)
    rest_cols = pl.ds(main, total_width - main)

    def add(ms, at, count, cols):
        here = pl.ds(PRIOR + at, count)
        total = None
        for m in ms:
            values = x_own[pl.ds(at, count), :] if m == 0 else buf[m, pl.ds(at, count), :]
            term = jnp.dot(values, weights_of(m, cols), preferred_element_type=F32)
            total = term if total is None else total + term
        if 0 not in ms:
            total = total + raw[here, cols]
        raw[here, cols] = total

    near = [m for m in range(1, n) if m == 1]
    far = sorted(range(2, n), key=lambda m: (-low_bit(m), m))
    step = 2 * BLOCK if tokens % (2 * BLOCK) == 0 else BLOCK
    for at in range(0, tokens, step):
        add([0], at, step, every)
    for at in range(0, tokens, step):
        for m in near:
            for c in range(at // PIECE, (at + step) // PIECE):
                arrive(m, c)
            add([m], at, step, every)

    within = row >= col
    before = row > col
    eye = (row == col).astype(F32)
    lower = within.astype(F32).astype(BF16)
    lower3 = jnp.concatenate([lower, lower, lower], axis=1)
    lane = lax.broadcasted_iota(jnp.int32, (1, LANES), 1)
    offset = jnp.zeros((1, LANES), F32)
    rate = jnp.zeros((1, LANES), F32)
    for h in range(heads):
        offset = jnp.where(lane == h, beta_bias[h], offset)
        offset = jnp.where(lane == heads + h, decay_bias[h], offset)
        rate = jnp.where(lane == heads + h, rates[h], rate)
    rate = -jnp.exp(rate)
    tiles = BLOCK // BASE
    tile_shape = (tiles, BASE, BLOCK)
    on_tile = (
        lax.broadcasted_iota(jnp.int32, tile_shape, 0)
        == lax.broadcasted_iota(jnp.int32, tile_shape, 2) // BASE
    )
    small_eye = (
        lax.broadcasted_iota(jnp.int32, (BASE, BLOCK), 0)
        == lax.broadcasted_iota(jnp.int32, (BASE, BLOCK), 1) % BASE
    ).astype(F32)

    def add_prior():
        @pl.when(has_before)
        def _():
            total = jnp.zeros((PRIOR, total_width), F32)
            for m in range(n):
                tails[m].wait_recv()
                total = total + jnp.dot(prior[m], weights_of(m, every), preferred_element_type=F32)
            raw[pl.ds(0, PRIOR), :] = total

        @pl.when(jnp.logical_not(has_before))
        def _():
            raw[pl.ds(0, PRIOR), :] = jnp.zeros((PRIOR, total_width), F32)

    def mixed(kind, h, b):
        base = (q_at, 0, width)[kind] + h * dim
        start = PRIOR + b * BLOCK
        total = None
        for s in range(taps.shape[1]):
            tap = taps[kind, pl.ds(s, 1), pl.ds(h * dim, dim)]
            term = tap * raw[pl.ds(start - s, BLOCK), pl.ds(base, dim)]
            total = term if total is None else total + term
        return total * jax.nn.sigmoid(total)

    def unit(values):
        return values * lax.rsqrt(jnp.sum(values * values, axis=-1, keepdims=True) + 1.0)

    def bases(lows):
        stack = []
        for low in lows:
            packed = jnp.sum(jnp.where(on_tile, low.reshape(tile_shape), 0.0), axis=0)
            high = packed.astype(BF16).astype(F32)
            stack += [high, packed - high]
        found = dot(jnp.concatenate(stack, axis=0), spread[...])
        results = []
        for h in range(len(lows)):
            inverse = small_eye
            for j in range(BASE - 1):
                cols = slice(j * LANES, (j + 1) * LANES)
                at = 2 * BASE * h
                factor = found[at : at + BASE, cols] + found[at + BASE : at + 2 * BASE, cols]
                inverse = inverse - factor * inverse[j : j + 1, :]
            results.append(
                jnp.where(on_tile, inverse[None], 0.0).reshape(BLOCK, BLOCK)
            )
        return results

    def small_terms(b):
        small = raw[pl.ds(PRIOR + b * BLOCK, BLOCK), pl.ds(2 * width, LANES)] + offset
        betas = jax.nn.sigmoid(small)
        steps = rate * (jnp.maximum(small, 0.0) + jnp.log1p(jnp.exp(-jnp.abs(small))))
        one, rest = split(steps)
        left = steps - one.astype(F32) - rest.astype(F32)
        run = dot(lower3, jnp.concatenate([one, rest, left.astype(BF16)], axis=0))
        return betas, run, run.T

    def block_terms(b, before_slab, midway):
        betas, run, across = small_terms(b)
        keys, decays, growths, lows, weighteds, ends = [], [], [], [], [], []
        sides = []
        for h in range(heads):
            k = unit(mixed(1, h, b))
            down = run[:, heads + h : heads + h + 1]
            along = across[heads + h : heads + h + 1, :]
            beta = betas[:, h : h + 1]
            last = down[BLOCK - 1 : BLOCK, :]
            decay = jnp.where(within, jnp.exp(jnp.minimum(down - along, 0.0)), 0.0)
            key = split(k)
            gram = dot3(key, key, ((1,), (1,)))
            lows.append(jnp.where(before, beta * decay * gram, 0.0))
            keys.append(key)
            decays.append(decay)
            growth = jnp.exp(down)
            growths.append(growth)
            ends.append(jnp.exp(last))
            weighteds.append((jnp.exp(last - down) * k).T)
        inverses = bases(lows)
        for h in range(heads):
            beta = betas[:, h : h + 1]
            v = mixed(2, h, b)
            scale = beta * growths[h]
            if before_slab is None:
                k = keys[h][0].astype(F32) + keys[h][1].astype(F32)
                sides.append(jnp.concatenate([-scale * k, beta * v], axis=1))
            else:
                moved = -scale * dot3(keys[h], before_slab[h])
                sides.append(
                    jnp.concatenate([moved[:, :dim], moved[:, dim:] + beta * v], axis=1)
                )
        span = BASE
        while 4 * span < BLOCK:
            area = (row // (4 * span) == col // (4 * span)) & (row // span > col // span)
            shares = [split(inv) for inv in inverses]
            links = [
                split(dot3(share, jnp.where(area, low, 0.0))) for share, low in zip(shares, lows)
            ]
            nexts = []
            for inv, share, link in zip(inverses, shares, links):
                pair = dot3(link, tuple(
                    jnp.concatenate([a, c], axis=1) for a, c in zip(share, link)
                ))
                nexts.append((inv - pair[:, :BLOCK], pair[:, BLOCK:]))
            inverses = [z + dot3(square, z) for z, square in nexts]
            span *= 4
        midway()
        area = row // span > col // span
        wide = [
            dot3(inv, jnp.concatenate([jnp.where(area, low, 0.0), side], axis=1))
            for inv, low, side in zip(inverses, lows, sides)
        ]
        links = [split(got[:, :BLOCK]) for got in wide]
        solved = [got[:, BLOCK:] for got in wide]
        level = span
        while level < BLOCK:
            nexts = []
            for link, have in zip(links, solved):
                share = split(have)
                more = level * 2 < BLOCK
                right = tuple(
                    jnp.concatenate([a, c], axis=1) for a, c in zip(share, link)
                ) if more else share
                got = dot3(link, right)
                nexts.append((got[:, : 2 * dim], got[:, 2 * dim :] if more else None))
            sign = -1.0 if level == span else 1.0
            solved = [have + sign * got for have, (got, _) in zip(solved, nexts)]
            links = [split(square) if square is not None else None for _, square in nexts]
            level *= 2
        slabs = []
        shares = [split(have) for have in solved]
        for h in range(heads):
            got = dot3(weighteds[h], shares[h])
            if before_slab is None:
                slabs.append(jnp.concatenate([ends[h] * eye + got[:, :dim], got[:, dim:]], axis=1))
            else:
                high, rest = before_slab[h]
                have = high.astype(F32) + rest.astype(F32)
                slabs.append(ends[h] * have + got)

        def outputs():
            for h in range(heads):
                q = unit(mixed(0, h, b))
                mix = decays[h] * dot3(q, keys[h], ((1,), (1,)))
                lead = growths[h] * q
                if before_slab is None:
                    got = dot3(mix, shares[h])
                    read, here = got[:, :dim] + lead, got[:, dim:]
                else:
                    right = tuple(
                        jnp.concatenate([a, c], axis=0)
                        for a, c in zip(shares[h], before_slab[h])
                    )
                    got = dot3(jnp.concatenate([mix, lead], axis=1), right)
                    read, here = got[:, :dim], got[:, dim:]
                reader[h, b] = read.astype(BF16)
                local[h, b] = here

        return slabs, outputs

    def columns_of(m):
        return pl.ds(pl.multiple_of((me ^ m) * columns, LANES), columns)

    own = pltpu.make_async_copy(w_ref.at[:, columns_of(0)], w_buf.at[0], own_sem)
    share = width // 2

    def part_of(which):
        return pl.ds(pl.multiple_of(which * share, share), share)

    moves, passes = {}, {}
    for m in range(1, n):
        if m in near:
            source, target = w_ref.at[:, columns_of(m)], w_buf.at[m]
        else:
            source, target = w_ref.at[part_of(odd), columns_of(m)], w_buf.at[m, part_of(odd)]
            passes[m] = remote(
                w_buf.at[m, part_of(odd)], w_buf.at[m, part_of(odd)], v_send.at[m], v_recv.at[m],
                (mate, me),
            )
        moves[m] = remote(source, target, w_send.at[m], w_recv.at[m], (seq, me ^ m))

    def arrive_block(b):
        for c in range(b * per_block, (b + 1) * per_block):
            for m in far:
                if low_bit(m) > 1:
                    arrive(m, c)

    direct = [m for m in far if low_bit(m) > 1]
    passed = [m for m in far if low_bit(m) == 1]
    slabs = None
    outputs = []
    add_prior()
    arrive_block(0)
    add(direct, 0, BLOCK, first_cols)
    for b in range(blocks):
        for m in passed:
            for c in range(b * per_block, (b + 1) * per_block):
                arrive(m, c)
        add(passed, b * BLOCK, BLOCK, first_cols)

        def midway():
            if b + 1 < blocks:
                arrive_block(b + 1)
                add(direct, (b + 1) * BLOCK, BLOCK, first_cols)
            if b + 2 == max(blocks, 2):
                own.start()
                for m in far + near:
                    moves[m].start()

        prior_slab = None if slabs is None else [split(value) for value in slabs]
        slabs, later = block_terms(b, prior_slab, midway)
        outputs.append(later)

    swaps_a, swaps_c = [], []
    for h in range(heads):
        slab_c[h] = slabs[h][:, dim:].astype(slab_c.dtype)
        slab_a[h] = slabs[h][:, :dim].astype(slab_a.dtype)
        swaps_a.append(
            remote(slab_a.at[h], mate_a.at[h], sa_send.at[h], sa_recv.at[h], (mate, me))
        )
        swaps_c.append(
            remote(slab_c.at[h], mate_c.at[h], sc_send.at[h], sc_recv.at[h], (mate, me))
        )
    for h in range(heads):

        @pl.when(gives_c[h])
        def _():
            swaps_c[h].start()

        @pl.when(gives_a[h])
        def _():
            swaps_a[h].start()

    blank = jnp.zeros((dim, dim), slab_a.dtype)
    for h in range(heads):

        @pl.when(jnp.logical_not(takes_a[h]))
        def _():
            mate_a[h] = blank

        @pl.when(jnp.logical_not(takes_c[h]))
        def _():
            mate_c[h] = blank
        pre_c[h] = jnp.zeros((dim, dim), F32)

    for at in range(0, tokens, step):
        add(far, at, step, rest_cols)
    for h in range(heads):
        place = pl.ds(PRIOR, tokens), pl.ds(g_at + h * dim, dim)
        gate = raw[place]
        raw[place] = gain[...] * (gate * jax.nn.sigmoid(gate))
    for later in outputs:
        later()

    def total_copy(source, target, send_sem, recv_sem, r, h, j):
        return remote(
            source.at[r, h], target.at[r, h], send_sem.at[r, h, j], recv_sem.at[r, h],
            (seq + 2 + 2 * j, me),
        )

    totals_c, totals_a = {}, {}
    for r, half in enumerate(rounds):
        for h in range(heads):
            for j in range(half // 2):
                totals_c[r, h, j] = total_copy(go_c, in_c, c_send, c_recv, r, h, j)
                totals_a[r, h, j] = total_copy(go_a, in_a, a_send, a_recv, r, h, j)
    asides = {
        h: remote(go_c.at[0, h], in_c.at[0, h], side_send.at[h], c_recv.at[0, h], (seq + 1, me))
        for h in range(lone, heads) if rounds
    }
    pair_a, pair_c, firsts = [], [], []

    def giver(r, h):
        return sources[r] & (seq != 0) if r == 0 and h >= lone else sources[r]

    def send_total(r, h):
        @pl.when(giver(r, h))
        def _():
            total = pair_c[h] if r == 0 else dot(pair_a[h], pre_c[h]) + pair_c[h]
            go_c[r, h] = total.astype(go_c.dtype)
            for j in reversed(range(rounds[r] // 2)):
                totals_c[r, h, j].start()

            @pl.when(whole[r])
            def _():
                total = pair_a[h] if r == 0 else dot(pair_a[h], pre_a[h])
                go_a[r, h] = total.astype(go_a.dtype)
                for j in reversed(range(rounds[r] // 2)):
                    totals_a[r, h, j].start()

        if r == 0 and h in asides:

            @pl.when(starts)
            def _():
                asides[h].start()

    def take_total(r, h):
        first = seq % rounds[r] < 2

        @pl.when(uppers[r])
        def _():
            totals_c[r, h, 0].wait_recv()

            @pl.when(first)
            def _():
                pre_c[h] = in_c[r, h].astype(F32)

            @pl.when(jnp.logical_not(first))
            def _():
                pre_c[h] = dot(pre_a[h], in_c[r, h]) + pre_c[h]

            @pl.when(whole[r])
            def _():
                totals_a[r, h, 0].wait_recv()

                @pl.when(first)
                def _():
                    pre_a[h] = in_a[r, h].astype(F32)

                @pl.when(jnp.logical_not(first))
                def _():
                    pre_a[h] = dot(pre_a[h], in_a[r, h])

    def hand_over():
        for m in passes:
            moves[m].wait_recv()
            passes[m].start()

    lifts = {}

    def lift(m, bit, h, b):
        got = m | bit
        return remote(
            hid.at[m, h, b], hid.at[got, h, b],
            h_send.at[got, h, b], h_recv.at[got, h, b], (seq, me ^ bit),
        )

    def forward(m, h, b):
        limit = n if m == 0 else low_bit(m)
        for bit in bits:
            if bit < limit:
                lifts[m | bit, h, b] = lift(m, bit, h, b)
                lifts[m | bit, h, b].start()

    states = []

    def read(h, b):
        head_out = dot(reader[h, b], states[h]) + local[h, b]
        gate = raw[pl.ds(PRIOR + b * BLOCK, BLOCK), pl.ds(g_at + h * dim, dim)]
        scaled = head_out * lax.rsqrt(
            jnp.mean(head_out * head_out, axis=-1, keepdims=True) + norm_floor
        )
        hid[0, h, b] = (scaled * gate).astype(BF16)
        forward(0, h, b)

    for h in range(heads):
        @pl.when(takes_c[h])
        def _():
            swaps_c[h].wait_recv()

        @pl.when(takes_a[h])
        def _():
            swaps_a[h].wait_recv()

        here_a, here_c = slab_a[h].astype(F32), slab_c[h].astype(F32)
        there_a, there_c = mate_a[h].astype(F32), mate_c[h].astype(F32)
        left = jnp.where(is_odd, here_a, there_a)
        right_a = jnp.where(is_odd, there_a, here_a)
        right_c = jnp.where(is_odd, there_c, here_c)
        back_c = jnp.where(is_odd, here_c, there_c)
        moved = dot(left, jnp.concatenate([right_a, right_c], axis=1))
        pair_a.append(moved[:, :dim])
        pair_c.append(moved[:, dim:] + back_c)
        firsts.append((right_a, right_c))
        if rounds:
            send_total(0, h)

    upper = uppers[-1] if rounds else seq < 0

    @pl.when(upper)
    def _():
        hand_over()

    for r in range(len(rounds) - 1):
        for h in range(heads):
            take_total(r, h)
            send_total(r + 1, h)

    for h in range(heads):
        if rounds:
            take_total(len(rounds) - 1, h)
        first_a, first_c = firsts[h]
        state = pre_c[h]
        states.append(jnp.where(is_odd, dot(first_a, state) + first_c, state))
        if h + 1 < heads:
            for b in range(blocks // 2):
                read(h, b)

    @pl.when(jnp.logical_not(upper))
    def _():
        hand_over()

    for b in range(blocks):
        for h in range(heads):
            if h + 1 == heads or b >= blocks // 2:
                read(h, b)

    own.wait()
    for m in near:
        moves[m].wait_recv()
    order = sorted(range(1, n), key=lambda m: (m != 1, -low_bit(m), m))

    def rows_of(m, b):
        return jnp.concatenate([hid[m, h, b] for h in range(heads)], axis=1)

    for b in range(blocks):
        total = jnp.dot(rows_of(0, b), w_buf[0], preferred_element_type=F32)
        for m in order:
            if b == 0 and m in passes:
                passes[m].wait_recv()
            for h in range(heads):
                lifts[m, h, b].wait_recv()
                forward(m, h, b)
            total = total + jnp.dot(rows_of(m, b), w_buf[m], preferred_element_type=F32)
        out_ref[pl.ds(b * BLOCK, BLOCK), :] = total.astype(BF16)

    for copies in (hops, lifts, moves, passes):
        for copy in copies.values():
            copy.wait_send()

    for h in range(heads):

        @pl.when(gives_c[h])
        def _():
            swaps_c[h].wait_send()

        @pl.when(gives_a[h])
        def _():
            swaps_a[h].wait_send()

        if h in asides:

            @pl.when(starts)
            def _():
                asides[h].wait_send()

        for r, half in enumerate(rounds):

            @pl.when(giver(r, h))
            def _():
                for j in range(half // 2):
                    totals_c[r, h, j].wait_send()

                @pl.when(whole[r])
                def _():
                    for j in range(half // 2):
                        totals_a[r, h, j].wait_send()

    @pl.when(has_next)
    def _():
        for tail in tails:
            tail.wait_send()


def on_device(
    seqs, n,
    layer_in, query_weight, key_weight, value_weight, gate_weight, beta_weight, decay_weight,
    conv_weight, decay_log, beta_bias, decay_bias, norm_gain, out_weight,
):
    tokens, feats = layer_in.shape
    model, width = query_weight.shape
    heads = beta_weight.shape[1]
    dim = width // heads
    blocks = tokens // BLOCK
    pieces = tokens // PIECE
    total_width = 4 * width + LANES
    columns = out_weight.shape[1] // n
    vmem = pl.BlockSpec(memory_space=pltpu.VMEM)
    anywhere = pl.BlockSpec(memory_space=pl.ANY)
    dma = pltpu.SemaphoreType.DMA
    wire = BF16 if seqs <= 8 else F32
    steps = max(1, len(rounds_of(seqs)))
    most = max(1, seqs // 4)
    square = pltpu.VMEM((heads, dim, dim), wire)
    stage = pltpu.VMEM((steps, heads, dim, dim), wire)
    total = pltpu.VMEM((heads, dim, dim), F32)
    return pl.pallas_call(
        functools.partial(layer_kernel, seqs, n, heads),
        out_shape=pltpu.VMEM((tokens, columns), BF16),
        in_specs=[anywhere] * 13,
        out_specs=vmem,
        scratch_shapes=[
            pltpu.VMEM((model, total_width), BF16),
            pltpu.VMEM((LANES, model), F32),
            pltpu.VMEM((LANES, (BASE - 1) * LANES), BF16),
            pltpu.VMEM((tokens, feats), BF16),
            pltpu.VMEM((n, tokens, feats), BF16),
            pltpu.VMEM((n, PRIOR, feats), BF16),
            pltpu.VMEM((PRIOR + tokens, total_width), F32),
            pltpu.VMEM((heads, blocks, BLOCK, dim), F32),
            pltpu.VMEM((heads, blocks, BLOCK, dim), BF16),
            square, square, square, square,
            stage, stage, stage, stage,
            total, total,
            pltpu.VMEM((n, width, columns), BF16),
            pltpu.VMEM((n, heads, blocks, BLOCK, dim), BF16),
            pltpu.VMEM((heads, model), BF16),
            pltpu.VMEM((heads, model), BF16),
            pltpu.VMEM((conv_weight.shape[1], conv_weight.shape[0], width), F32),
            pltpu.VMEM((1, dim), F32),
            pltpu.SMEM((heads,), F32),
            pltpu.SMEM((heads,), F32),
            pltpu.SMEM((heads,), F32),
            dma((4,)),
            dma((7,)),
            dma(()),
            dma((n, pieces)),
            dma((n, pieces)),
            dma((n,)),
            dma((n,)),
            dma(()),
            dma((n,)),
            dma((n,)),
            dma((n,)),
            dma((n,)),
            dma((heads,)),
            dma((heads,)),
            dma((heads,)),
            dma((heads,)),
            dma((heads,)),
            dma((steps, heads, most)),
            dma((steps, heads)),
            dma((steps, heads, most)),
            dma((steps, heads)),
            dma((n, heads, blocks)),
            dma((n, heads, blocks)),
        ],
        compiler_params=pltpu.CompilerParams(
            collective_id=0, has_side_effects=True, vmem_limit_bytes=60 * 1024 * 1024
        ),
    )(
        layer_in, query_weight, key_weight, value_weight, gate_weight,
        beta_weight.T, decay_weight.T, conv_weight.transpose(1, 0, 2),
        decay_log, beta_bias, decay_bias, norm_gain[None], out_weight,
    )


def solution(mesh):
    return jax.shard_map(
        functools.partial(on_device, mesh.shape["seq"], mesh.shape["head"]),
        mesh=mesh,
        in_specs=(
            P("seq", "head"),
            P(None, "head"),
            P(None, "head"),
            P(None, "head"),
            P(None, "head"),
            P(None, "head"),
            P(None, "head"),
            P(None, None, "head"),
            P("head"),
            P("head"),
            P("head"),
            P(),
            P("head", None),
        ),
        out_specs=P("seq", "head"),
        check_vma=False,
    )
```

```python
import functools

import jax
import jax.numpy as jnp
from jax import lax
from jax.experimental import pallas as pl
from jax.experimental.pallas import tpu as pltpu
from jax.sharding import PartitionSpec as P

BLOCK = 128
PRIOR = 8
LANES = 128
PIECE = 64
BASE = 8
MESH = pl.DeviceIdType.MESH
F32 = jnp.float32
BF16 = jnp.bfloat16
norm_floor = 0.0001


def bits_below(limit):
    found = []
    bit = limit // 2
    while bit:
        found.append(bit)
        bit //= 2
    return found


def low_bit(value):
    return value & -value


def rounds_of(seqs):
    found = []
    half = 2
    while half < seqs:
        found.append(half)
        half *= 2
    return found


def meet(peers):
    barrier = pltpu.get_barrier_semaphore()
    expected = 0
    for present, device in peers:
        if present is True:
            pl.semaphore_signal(barrier, inc=1, device_id=device, device_id_type=MESH)
            expected = expected + 1
        else:

            @pl.when(present)
            def _():
                pl.semaphore_signal(barrier, inc=1, device_id=device, device_id_type=MESH)

            expected = expected + present.astype(jnp.int32)
    pl.semaphore_wait(barrier, expected)


def remote(source, target, send_sem, recv_sem, device):
    return pltpu.make_async_remote_copy(
        src_ref=source,
        dst_ref=target,
        send_sem=send_sem,
        recv_sem=recv_sem,
        device_id=device,
        device_id_type=MESH,
    )


def dot(left, right, contract=((1,), (0,))):
    return lax.dot_general(
        left.astype(BF16), right.astype(BF16), (contract, ((), ())), preferred_element_type=F32
    )


def split(value):
    high = value.astype(BF16)
    return high, (value - high.astype(F32)).astype(BF16)


def dot3(left, right, contract=((1,), (0,))):
    lh, ll = left if isinstance(left, tuple) else split(left)
    rh, rl = right if isinstance(right, tuple) else split(right)
    axis = contract[1][0]
    both = dot(jnp.concatenate([lh, lh], axis=1), jnp.concatenate([rh, rl], axis=axis), contract)
    return both + dot(ll, rh, contract)


def layer_kernel(
    seqs, n, heads,
    x_ref, wq, wk, wv, wg, beta_in, step_in, taps_in, rates_in, bias_in, shift_in, gain_in, w_ref,
    out_ref,
    w_all, w_flat, spread, x_own, buf, prior, raw, local, reader,
    slab_a, slab_c, mate_a, mate_c, go_a, go_c, in_a, in_c, pre_a, pre_c,
    w_buf, hid, acc,
    beta_ref, step_ref, taps, gain, rates, beta_bias, decay_bias,
    load_sem, small_sem, x_sem, x_send, x_recv, p_send, p_recv, own_sem, w_send, w_recv,
    v_send, v_recv, sa_send, sa_recv, sc_send, sc_recv, side_send, a_send, a_recv, c_send, c_recv,
    h_send, h_recv,
):
    seq = lax.axis_index("seq")
    me = lax.axis_index("head")
    tokens, feats = x_ref.shape
    width = wq.shape[1]
    dim = LANES
    blocks = tokens // BLOCK
    columns = out_ref.shape[1]
    pieces = tokens // PIECE
    per_block = BLOCK // PIECE
    main = 2 * width + LANES
    total_width = w_all.shape[1]
    q_at = main
    g_at = main + width
    bits = bits_below(n)

    own_load = pltpu.make_async_copy(x_ref, x_own, x_sem)
    own_load.start()
    loads = []
    for w, at in ((wk, 0), (wv, width), (wq, q_at), (wg, g_at)):
        loads.append(pltpu.make_async_copy(w, w_all.at[:, pl.ds(at, width)], load_sem))
    smalls = [
        pltpu.make_async_copy(source, target, small_sem.at[i])
        for i, (source, target) in enumerate((
            (beta_in, beta_ref), (step_in, step_ref), (taps_in, taps), (gain_in, gain),
            (rates_in, rates), (bias_in, beta_bias), (shift_in, decay_bias),
        ))
    ]
    for load in smalls + loads:
        load.start()
    has_next = seq < seqs - 1
    has_before = seq > 0
    odd = seq % 2
    is_odd = odd == 1
    mate = seq + 1 - 2 * odd
    lone = heads // 2
    rounds = rounds_of(seqs)
    uppers, sources, origins, whole = [], [], [], []
    for half in rounds:
        inside = seq % (2 * half)
        uppers.append(inside >= half)
        sources.append(inside // 2 == half // 2 - 1)
        origins.append(seq - inside + half - 2 + odd)
        whole.append(seq - inside > 0)
    starts = seq == 1 if rounds else seq < 0
    gives_c = [seq >= 0 if h < lone else seq != 1 for h in range(heads)]
    gives_a = [seq != 0 if h < lone else seq >= 2 for h in range(heads)]
    takes_c = [seq >= 0 if h < lone else seq != 0 for h in range(heads)]
    takes_a = [seq != 1 if h < lone else seq >= 2 for h in range(heads)]
    peers = [(True, (seq, me ^ m)) for m in range(1, n)]
    peers += [(has_next, (seq + 1, me ^ m)) for m in range(n)]
    peers += [(has_before, (seq - 1, me ^ m)) for m in range(n)]
    for r, half in enumerate(rounds):
        peers += [(sources[r], (seq + 2 + 2 * j, me)) for j in range(half // 2)]
        peers += [(uppers[r], (origins[r], me))]
    meet(peers)
    own_load.wait()

    forwards = [m for m in range(1, n) if low_bit(m) > 1]
    lasts = [m for m in range(1, n) if low_bit(m) == 1]

    def slot_of(m, c):
        if m in forwards:
            return forwards.index(m) * pieces + c
        return len(forwards) * pieces + lasts.index(m) * blocks + c // per_block

    def hop(m, bit, c):
        piece = pl.ds(c * PIECE, PIECE)
        source = x_own.at[piece] if m == 0 else buf.at[m, piece]
        got = m | bit
        return remote(
            source, buf.at[got, piece], x_send.at[got - 1], x_recv.at[slot_of(got, c)],
            (seq, me ^ bit),
        )

    tails = [
        remote(
            x_own.at[pl.ds(tokens - PRIOR, PRIOR)],
            prior.at[m],
            p_send,
            p_recv,
            (seq + 1, me ^ m),
        )
        for m in range(n)
    ]

    @pl.when(has_next)
    def _():
        for tail in tails:
            tail.start()

    hops = {}
    for c in range(pieces):
        for bit in bits:
            hops[bit, c] = hop(0, bit, c)
            hops[bit, c].start()

    row = lax.broadcasted_iota(jnp.int32, (BLOCK, BLOCK), 0)
    col = lax.broadcasted_iota(jnp.int32, (BLOCK, BLOCK), 1)
    for j in range(BASE - 1):
        spread[:, pl.ds(j * LANES, LANES)] = (row == col // BASE * BASE + j).astype(F32).astype(BF16)

    for load in smalls:
        load.wait()
    w_flat[...] = jnp.zeros(w_flat.shape, F32)
    w_flat[pl.ds(0, heads), :] = beta_ref[...].astype(F32)
    w_flat[pl.ds(heads, heads), :] = step_ref[...].astype(F32)
    for i in range(w_flat.shape[1] // LANES):
        piece = pl.ds(i * LANES, LANES)
        w_all[piece, pl.ds(2 * width, LANES)] = w_flat[:, piece].T.astype(BF16)
    flat = w_all.at[:, pl.ds(0, len(loads) * width)]
    pltpu.make_async_copy(flat, flat, load_sem).wait()

    def weights_of(m, cols):
        start = pl.multiple_of((me ^ m) * feats, LANES)
        return w_all[pl.ds(start, feats), cols]

    def whole_block(m, b):
        return buf.at[m, pl.ds(b * BLOCK, BLOCK)]

    def arrive(m, b):
        if m in lasts:
            here = whole_block(m, b)
            remote(
                here, here, x_send.at[m - 1], x_recv.at[slot_of(m, b * per_block)], (seq, me ^ 1)
            ).wait_recv()
            return
        for c in range(b * per_block, (b + 1) * per_block):
            hops[m, c].wait_recv()
            for bit in bits:
                if bit < low_bit(m):
                    hops[m | bit, c] = hop(m, bit, c)
                    hops[m | bit, c].start()

    every = pl.ds(0, total_width)
    first_cols = pl.ds(0, main)
    rest_cols = pl.ds(main, total_width - main)

    def add(ms, at, count, cols):
        here = pl.ds(PRIOR + at, count)
        total = None
        for m in ms:
            values = x_own[pl.ds(at, count), :] if m == 0 else buf[m, pl.ds(at, count), :]
            term = jnp.dot(values, weights_of(m, cols), preferred_element_type=F32)
            total = term if total is None else total + term
        if 0 not in ms:
            total = total + raw[here, cols]
        raw[here, cols] = total

    near = [m for m in range(1, n) if m == 1]
    far = sorted(range(2, n), key=lambda m: (-low_bit(m), m))
    step = 2 * BLOCK if tokens % (2 * BLOCK) == 0 else BLOCK
    for at in range(0, tokens, step):
        add([0], at, step, every)
    for at in range(0, tokens, step):
        for m in near:
            for b in range(at // BLOCK, (at + step) // BLOCK):
                arrive(m, b)
            add([m], at, step, every)

    within = row >= col
    before = row > col
    eye = (row == col).astype(F32)
    lower = within.astype(F32).astype(BF16)
    lower3 = jnp.concatenate([lower, lower, lower], axis=1)
    lane = lax.broadcasted_iota(jnp.int32, (1, LANES), 1)
    offset = jnp.zeros((1, LANES), F32)
    rate = jnp.zeros((1, LANES), F32)
    for h in range(heads):
        offset = jnp.where(lane == h, beta_bias[h], offset)
        offset = jnp.where(lane == heads + h, decay_bias[h], offset)
        rate = jnp.where(lane == heads + h, rates[h], rate)
    rate = -jnp.exp(rate)
    tiles = BLOCK // BASE
    tile_shape = (tiles, BASE, BLOCK)
    on_tile = (
        lax.broadcasted_iota(jnp.int32, tile_shape, 0)
        == lax.broadcasted_iota(jnp.int32, tile_shape, 2) // BASE
    )
    small_eye = (
        lax.broadcasted_iota(jnp.int32, (BASE, BLOCK), 0)
        == lax.broadcasted_iota(jnp.int32, (BASE, BLOCK), 1) % BASE
    ).astype(F32)

    def add_prior():
        @pl.when(has_before)
        def _():
            total = jnp.zeros((PRIOR, total_width), F32)
            remote(prior, prior, p_send, p_recv, (seq - 1, me)).wait_recv()
            for m in range(n):
                total = total + jnp.dot(prior[m], weights_of(m, every), preferred_element_type=F32)
            raw[pl.ds(0, PRIOR), :] = total

        @pl.when(jnp.logical_not(has_before))
        def _():
            raw[pl.ds(0, PRIOR), :] = jnp.zeros((PRIOR, total_width), F32)

    def mixed(kind, h, b):
        base = (q_at, 0, width)[kind] + h * dim
        start = PRIOR + b * BLOCK
        total = None
        for s in range(taps.shape[1]):
            tap = taps[kind, pl.ds(s, 1), pl.ds(h * dim, dim)]
            term = tap * raw[pl.ds(start - s, BLOCK), pl.ds(base, dim)]
            total = term if total is None else total + term
        return total * jax.nn.sigmoid(total)

    def unit(values):
        return values * lax.rsqrt(jnp.sum(values * values, axis=-1, keepdims=True) + 1.0)

    def bases(lows):
        stack = []
        for low in lows:
            packed = jnp.sum(jnp.where(on_tile, low.reshape(tile_shape), 0.0), axis=0)
            high = packed.astype(BF16).astype(F32)
            stack += [high, packed - high]
        found = dot(jnp.concatenate(stack, axis=0), spread[...])
        results = []
        for h in range(len(lows)):
            inverse = small_eye
            for j in range(BASE - 1):
                cols = slice(j * LANES, (j + 1) * LANES)
                at = 2 * BASE * h
                factor = found[at : at + BASE, cols] + found[at + BASE : at + 2 * BASE, cols]
                inverse = inverse - factor * inverse[j : j + 1, :]
            results.append(
                jnp.where(on_tile, inverse[None], 0.0).reshape(BLOCK, BLOCK)
            )
        return results

    def small_terms(b):
        small = raw[pl.ds(PRIOR + b * BLOCK, BLOCK), pl.ds(2 * width, LANES)] + offset
        betas = jax.nn.sigmoid(small)
        steps = rate * (jnp.maximum(small, 0.0) + jnp.log1p(jnp.exp(-jnp.abs(small))))
        one, rest = split(steps)
        left = steps - one.astype(F32) - rest.astype(F32)
        run = dot(lower3, jnp.concatenate([one, rest, left.astype(BF16)], axis=0))
        return betas, run, run.T

    def block_terms(b, before_slab, midway):
        betas, run, across = small_terms(b)
        keys, decays, growths, lows, weighteds, ends = [], [], [], [], [], []
        sides = []
        for h in range(heads):
            k = unit(mixed(1, h, b))
            down = run[:, heads + h : heads + h + 1]
            along = across[heads + h : heads + h + 1, :]
            beta = betas[:, h : h + 1]
            last = down[BLOCK - 1 : BLOCK, :]
            decay = jnp.where(within, jnp.exp(jnp.minimum(down - along, 0.0)), 0.0)
            key = split(k)
            gram = dot3(key, key, ((1,), (1,)))
            lows.append(jnp.where(before, beta * decay * gram, 0.0))
            keys.append(key)
            decays.append(decay)
            growth = jnp.exp(down)
            growths.append(growth)
            ends.append(jnp.exp(last))
            weighteds.append((jnp.exp(last - down) * k).T)
        inverses = bases(lows)
        for h in range(heads):
            beta = betas[:, h : h + 1]
            v = mixed(2, h, b)
            scale = beta * growths[h]
            if before_slab is None:
                k = keys[h][0].astype(F32) + keys[h][1].astype(F32)
                sides.append(jnp.concatenate([-scale * k, beta * v], axis=1))
            else:
                moved = -scale * dot3(keys[h], before_slab[h])
                sides.append(
                    jnp.concatenate([moved[:, :dim], moved[:, dim:] + beta * v], axis=1)
                )
        span = BASE
        while 4 * span < BLOCK:
            area = (row // (4 * span) == col // (4 * span)) & (row // span > col // span)
            shares = [split(inv) for inv in inverses]
            links = [
                split(dot3(share, jnp.where(area, low, 0.0))) for share, low in zip(shares, lows)
            ]
            nexts = []
            for inv, share, link in zip(inverses, shares, links):
                pair = dot3(link, tuple(
                    jnp.concatenate([a, c], axis=1) for a, c in zip(share, link)
                ))
                nexts.append((inv - pair[:, :BLOCK], pair[:, BLOCK:]))
            inverses = [z + dot3(square, z) for z, square in nexts]
            span *= 4
        midway()
        area = row // span > col // span
        wide = [
            dot3(inv, jnp.concatenate([jnp.where(area, low, 0.0), side], axis=1))
            for inv, low, side in zip(inverses, lows, sides)
        ]
        links = [split(got[:, :BLOCK]) for got in wide]
        solved = [got[:, BLOCK:] for got in wide]
        level = span
        while level < BLOCK:
            nexts = []
            for link, have in zip(links, solved):
                share = split(have)
                more = level * 2 < BLOCK
                right = tuple(
                    jnp.concatenate([a, c], axis=1) for a, c in zip(share, link)
                ) if more else share
                got = dot3(link, right)
                nexts.append((got[:, : 2 * dim], got[:, 2 * dim :] if more else None))
            sign = -1.0 if level == span else 1.0
            solved = [have + sign * got for have, (got, _) in zip(solved, nexts)]
            links = [split(square) if square is not None else None for _, square in nexts]
            level *= 2
        slabs = []
        shares = [split(have) for have in solved]
        for h in range(heads):
            got = dot3(weighteds[h], shares[h])
            if before_slab is None:
                slabs.append(jnp.concatenate([ends[h] * eye + got[:, :dim], got[:, dim:]], axis=1))
            else:
                high, rest = before_slab[h]
                have = high.astype(F32) + rest.astype(F32)
                slabs.append(ends[h] * have + got)

        def outputs():
            for h in range(heads):
                q = unit(mixed(0, h, b))
                mix = decays[h] * dot3(q, keys[h], ((1,), (1,)))
                lead = growths[h] * q
                if before_slab is None:
                    got = dot3(mix, shares[h])
                    read, here = got[:, :dim] + lead, got[:, dim:]
                else:
                    right = tuple(
                        jnp.concatenate([a, c], axis=0)
                        for a, c in zip(shares[h], before_slab[h])
                    )
                    got = dot3(jnp.concatenate([mix, lead], axis=1), right)
                    read, here = got[:, :dim], got[:, dim:]
                reader[h, b] = read.astype(BF16)
                local[h, b] = here

        return slabs, outputs

    def columns_of(m):
        return pl.ds(pl.multiple_of((me ^ m) * columns, LANES), columns)

    own = pltpu.make_async_copy(w_ref.at[:, columns_of(0)], w_buf.at[0], own_sem)
    share = width // 2

    def part_of(which):
        return pl.ds(pl.multiple_of(which * share, share), share)

    moves, passes = {}, {}
    for m in range(1, n):
        if m in near:
            source, target = w_ref.at[:, columns_of(m)], w_buf.at[m]
        else:
            source, target = w_ref.at[part_of(odd), columns_of(m)], w_buf.at[m, part_of(odd)]
            passes[m] = remote(
                w_buf.at[m, part_of(odd)], w_buf.at[m, part_of(odd)], v_send, v_recv, (mate, me)
            )
        moves[m] = remote(
            source, target, w_send, w_recv.at[0 if m in near else 1], (seq, me ^ m)
        )
    half_slots = w_buf.at[pl.ds(0, len(passes) // 2)]
    all_halves = remote(half_slots, half_slots, v_send, v_recv, (mate, me))
    far_halves = remote(half_slots, half_slots, w_send, w_recv.at[1], (seq, me ^ n // 2))
    all_slots = w_buf.at[pl.ds(0, len(passes) // 2 + len(near))]
    all_moves = remote(all_slots, all_slots, w_send, w_recv.at[0], (seq, me ^ 1))

    def arrive_block(b):
        for m in far:
            if low_bit(m) > 1:
                arrive(m, b)

    direct = [m for m in far if low_bit(m) > 1]
    passed = [m for m in far if low_bit(m) == 1]
    slabs = None
    outputs = []
    add_prior()
    arrive_block(0)
    add(direct, 0, BLOCK, first_cols)
    for b in range(blocks):
        for m in passed:
            arrive(m, b)
        add(passed, b * BLOCK, BLOCK, first_cols)

        def midway():
            if b + 1 < blocks:
                arrive_block(b + 1)
                add(direct, (b + 1) * BLOCK, BLOCK, first_cols)
            if b + 2 == max(blocks, 2):
                own.start()
                for m in far + near:
                    moves[m].start()

        prior_slab = None if slabs is None else [split(value) for value in slabs]
        slabs, later = block_terms(b, prior_slab, midway)
        outputs.append(later)

    swaps_a, swaps_c = [], []
    for h in range(heads):
        slab_c[h] = slabs[h][:, dim:].astype(slab_c.dtype)
        slab_a[h] = slabs[h][:, :dim].astype(slab_a.dtype)
        swaps_a.append(
            remote(slab_a.at[h], mate_a.at[h], sa_send.at[h], sa_recv.at[h], (mate, me))
        )
        swaps_c.append(
            remote(slab_c.at[h], mate_c.at[h], sc_send.at[h], sc_recv.at[h], (mate, me))
        )
    for h in range(heads):

        @pl.when(gives_c[h])
        def _():
            swaps_c[h].start()

        @pl.when(gives_a[h])
        def _():
            swaps_a[h].start()

    blank = jnp.zeros((dim, dim), slab_a.dtype)
    for h in range(heads):

        @pl.when(jnp.logical_not(takes_a[h]))
        def _():
            mate_a[h] = blank

        @pl.when(jnp.logical_not(takes_c[h]))
        def _():
            mate_c[h] = blank
        pre_c[h] = jnp.zeros((dim, dim), F32)

    for at in range(0, tokens, step):
        add(far, at, step, rest_cols)
    for h in range(heads):
        place = pl.ds(PRIOR, tokens), pl.ds(g_at + h * dim, dim)
        gate = raw[place]
        raw[place] = gain[...] * (gate * jax.nn.sigmoid(gate))
    for later in outputs:
        later()

    def total_copy(source, target, send_sem, recv_sem, r, h, j):
        return remote(
            source.at[r, h], target.at[r, h], send_sem.at[rounds[r] // 2 - 1 + j, h],
            recv_sem.at[r, h], (seq + 2 + 2 * j, me),
        )

    totals_c, totals_a = {}, {}
    for r, half in enumerate(rounds):
        for h in range(heads):
            for j in range(half // 2):
                totals_c[r, h, j] = total_copy(go_c, in_c, c_send, c_recv, r, h, j)
                if r + 1 < len(rounds):
                    totals_a[r, h, j] = total_copy(go_a, in_a, a_send, a_recv, r, h, j)
    asides = {
        h: remote(go_c.at[0, h], in_c.at[0, h], side_send.at[h - lone], c_recv.at[0, h], (seq + 1, me))
        for h in range(lone, heads) if rounds
    }
    pair_a, pair_c, firsts = [], [], []

    def giver(r, h):
        return sources[r] & (seq != 0) if r == 0 and h >= lone else sources[r]

    def send_total(r, h):
        @pl.when(giver(r, h))
        def _():
            total = pair_c[h] if r == 0 else dot(pair_a[h], pre_c[h]) + pair_c[h]
            go_c[r, h] = total.astype(go_c.dtype)
            for j in reversed(range(rounds[r] // 2)):
                totals_c[r, h, j].start()

            if r + 1 == len(rounds):
                return

            @pl.when(whole[r])
            def _():
                total = pair_a[h] if r == 0 else dot(pair_a[h], pre_a[h])
                go_a[r, h] = total.astype(go_a.dtype)
                for j in reversed(range(rounds[r] // 2)):
                    totals_a[r, h, j].start()

        if r == 0 and h in asides:

            @pl.when(starts)
            def _():
                asides[h].start()

    def take_total(r, h):
        first = seq % rounds[r] < 2

        @pl.when(uppers[r])
        def _():
            totals_c[r, h, 0].wait_recv()

            @pl.when(first)
            def _():
                pre_c[h] = in_c[r, h].astype(F32)

            @pl.when(jnp.logical_not(first))
            def _():
                pre_c[h] = dot(pre_a[h], in_c[r, h]) + pre_c[h]

            if r + 1 == len(rounds):
                return

            @pl.when(whole[r])
            def _():
                totals_a[r, h, 0].wait_recv()

                @pl.when(first)
                def _():
                    pre_a[h] = in_a[r, h].astype(F32)

                @pl.when(jnp.logical_not(first))
                def _():
                    pre_a[h] = dot(pre_a[h], in_a[r, h])

    def hand_over():
        far_halves.wait_recv()
        for m in passes:
            passes[m].start()

    lifts = {}

    def lift_slot(m, h, b):
        if m in forwards:
            return (forwards.index(m) * blocks + b) * heads + h
        return (len(forwards) * heads + lasts.index(m)) * blocks + b

    def lift(m, bit, h, b):
        got = m | bit
        return remote(
            hid.at[m, b, h], hid.at[got, b, h],
            h_send.at[got - 1], h_recv.at[lift_slot(got, h, b)], (seq, me ^ bit),
        )

    def forward(m, h, b):
        limit = n if m == 0 else low_bit(m)
        for bit in bits:
            if bit < limit:
                lifts[m | bit, h, b] = lift(m, bit, h, b)
                lifts[m | bit, h, b].start()

    states = []

    def read(h, b):
        head_out = dot(reader[h, b], states[h]) + local[h, b]
        gate = raw[pl.ds(PRIOR + b * BLOCK, BLOCK), pl.ds(g_at + h * dim, dim)]
        scaled = head_out * lax.rsqrt(
            jnp.mean(head_out * head_out, axis=-1, keepdims=True) + norm_floor
        )
        hid[0, b, h] = (scaled * gate).astype(BF16)
        forward(0, h, b)

    for h in range(heads):
        @pl.when(takes_c[h])
        def _():
            swaps_c[h].wait_recv()

        @pl.when(takes_a[h])
        def _():
            swaps_a[h].wait_recv()

        here_a, here_c = slab_a[h].astype(F32), slab_c[h].astype(F32)
        there_a, there_c = mate_a[h].astype(F32), mate_c[h].astype(F32)
        left = jnp.where(is_odd, here_a, there_a)
        right_a = jnp.where(is_odd, there_a, here_a)
        right_c = jnp.where(is_odd, there_c, here_c)
        back_c = jnp.where(is_odd, here_c, there_c)
        moved = dot(left, jnp.concatenate([right_a, right_c], axis=1))
        pair_a.append(moved[:, :dim])
        pair_c.append(moved[:, dim:] + back_c)
        firsts.append((right_a, right_c))
        if rounds:
            send_total(0, h)

    upper = uppers[-1] if rounds else seq < 0

    @pl.when(upper)
    def _():
        hand_over()

    def relay(h):
        for r in range(len(rounds) - 1):
            take_total(r, h)
            send_total(r + 1, h)

    relay(0)
    for h in range(heads):
        if h == 0:

            @pl.when(jnp.logical_not(upper))
            def _():
                for other in range(1, heads):
                    relay(other)
                hand_over()

        else:

            @pl.when(upper)
            def _():
                relay(h)

        if rounds:
            take_total(len(rounds) - 1, h)
        first_a, first_c = firsts[h]
        state = pre_c[h]
        states.append(jnp.where(is_odd, dot(first_a, state) + first_c, state))
        for b in range(blocks):
            read(h, b)

    own.wait()
    for m in near:
        moves[m].wait_recv()

    def rows_of(m, b):
        return jnp.concatenate([hid[m, b, h] for h in range(heads)], axis=1)

    def settle(m, b):
        here = hid.at[m, b]
        remote(
            here, here, h_send.at[m - 1], h_recv.at[lift_slot(m, 0, b)], (seq, me ^ 1)
        ).wait_recv()

    for h in range(heads):
        for b in range(blocks):
            for m in forwards:
                lifts[m, h, b].wait_recv()
                forward(m, h, b)
            if h + 1 == heads:
                total = jnp.dot(rows_of(0, b), w_buf[0], preferred_element_type=F32)
                for m in near:
                    settle(m, b)
                    total = total + jnp.dot(rows_of(m, b), w_buf[m], preferred_element_type=F32)
                acc[b] = total
    all_halves.wait_recv()
    for b in range(blocks):
        total = acc[b]
        for m in far:
            if m in lasts:
                settle(m, b)
            total = total + jnp.dot(rows_of(m, b), w_buf[m], preferred_element_type=F32)
        out_ref[pl.ds(b * BLOCK, BLOCK), :] = total.astype(BF16)

    for m in range(1, n):
        remote(buf.at[m], buf.at[m], x_send.at[m - 1], x_recv.at[0], (seq, me ^ 1)).wait_send()
        remote(hid.at[m], hid.at[m], h_send.at[m - 1], h_recv.at[0], (seq, me ^ 1)).wait_send()
    all_moves.wait_send()
    all_halves.wait_send()

    for h in range(heads):

        @pl.when(gives_c[h])
        def _():
            swaps_c[h].wait_send()

        @pl.when(gives_a[h])
        def _():
            swaps_a[h].wait_send()

        if h in asides:

            @pl.when(starts)
            def _():
                asides[h].wait_send()

        for r, half in enumerate(rounds):

            @pl.when(giver(r, h))
            def _():
                for j in range(half // 2):
                    totals_c[r, h, j].wait_send()

                if r + 1 == len(rounds):
                    return

                @pl.when(whole[r])
                def _():
                    for j in range(half // 2):
                        totals_a[r, h, j].wait_send()

    @pl.when(has_next)
    def _():
        remote(prior, prior, p_send, p_recv, (seq + 1, me)).wait_send()


def on_device(
    seqs, n,
    layer_in, query_weight, key_weight, value_weight, gate_weight, beta_weight, decay_weight,
    conv_weight, decay_log, beta_bias, decay_bias, norm_gain, out_weight,
):
    tokens, feats = layer_in.shape
    model, width = query_weight.shape
    heads = beta_weight.shape[1]
    dim = width // heads
    blocks = tokens // BLOCK
    per_block = BLOCK // PIECE
    ways = (n // 2 - 1) * blocks
    total_width = 4 * width + LANES
    columns = out_weight.shape[1] // n
    vmem = pl.BlockSpec(memory_space=pltpu.VMEM)
    anywhere = pl.BlockSpec(memory_space=pl.ANY)
    dma = pltpu.SemaphoreType.DMA
    wire = BF16 if seqs <= 8 else F32
    steps = max(1, len(rounds_of(seqs)))
    most = max(1, seqs // 4)
    square = pltpu.VMEM((heads, dim, dim), wire)
    stage = pltpu.VMEM((steps, heads, dim, dim), wire)
    total = pltpu.VMEM((heads, dim, dim), F32)
    return pl.pallas_call(
        functools.partial(layer_kernel, seqs, n, heads),
        out_shape=pltpu.VMEM((tokens, columns), BF16),
        in_specs=[anywhere] * 13,
        out_specs=vmem,
        scratch_shapes=[
            pltpu.VMEM((model, total_width), BF16),
            pltpu.VMEM((LANES, model), F32),
            pltpu.VMEM((LANES, (BASE - 1) * LANES), BF16),
            pltpu.VMEM((tokens, feats), BF16),
            pltpu.VMEM((n, tokens, feats), BF16),
            pltpu.VMEM((n, PRIOR, feats), BF16),
            pltpu.VMEM((PRIOR + tokens, total_width), F32),
            pltpu.VMEM((heads, blocks, BLOCK, dim), F32),
            pltpu.VMEM((heads, blocks, BLOCK, dim), BF16),
            square, square, square, square,
            stage, stage, stage, stage,
            total, total,
            pltpu.VMEM((n, width, columns), BF16),
            pltpu.VMEM((n, blocks, heads, BLOCK, dim), BF16),
            pltpu.VMEM((blocks, BLOCK, columns), F32),
            pltpu.VMEM((heads, model), BF16),
            pltpu.VMEM((heads, model), BF16),
            pltpu.VMEM((conv_weight.shape[1], conv_weight.shape[0], width), F32),
            pltpu.VMEM((1, dim), F32),
            pltpu.SMEM((heads,), F32),
            pltpu.SMEM((heads,), F32),
            pltpu.SMEM((heads,), F32),
            dma(()),
            dma((7,)),
            dma(()),
            dma((n - 1,)),
            dma((ways * per_block + n // 2 * blocks,)),
            dma(()),
            dma(()),
            dma(()),
            dma(()),
            dma((2,)),
            dma(()),
            dma(()),
            dma((heads,)),
            dma((heads,)),
            dma((heads,)),
            dma((heads,)),
            dma((heads - heads // 2,)),
            dma((max(1, seqs // 4 - 1), heads)),
            dma((max(1, steps - 1), heads)),
            dma((max(1, seqs // 2 - 1), heads)),
            dma((steps, heads)),
            dma((n - 1,)),
            dma((ways * heads + n // 2 * blocks,)),
        ],
        compiler_params=pltpu.CompilerParams(
            collective_id=0, has_side_effects=True, vmem_limit_bytes=60 * 1024 * 1024
        ),
    )(
        layer_in, query_weight, key_weight, value_weight, gate_weight,
        beta_weight.T, decay_weight.T, conv_weight.transpose(1, 0, 2),
        decay_log, beta_bias, decay_bias, norm_gain[None], out_weight,
    )


def solution(mesh):
    return jax.shard_map(
        functools.partial(on_device, mesh.shape["seq"], mesh.shape["head"]),
        mesh=mesh,
        in_specs=(
            P("seq", "head"),
            P(None, "head"),
            P(None, "head"),
            P(None, "head"),
            P(None, "head"),
            P(None, "head"),
            P(None, "head"),
            P(None, None, "head"),
            P("head"),
            P("head"),
            P("head"),
            P(),
            P("head", None),
        ),
        out_specs=P("seq", "head"),
        check_vma=False,
    )
```

```python
import functools

import jax
import jax.numpy as jnp
from jax import lax
from jax.experimental import pallas as pl
from jax.experimental.pallas import tpu as pltpu
from jax.sharding import PartitionSpec as P

BLOCK = 128
PRIOR = 8
LANES = 128
PIECE = 64
BASE = 8

LAG = 2
MESH = pl.DeviceIdType.MESH
F32 = jnp.float32
BF16 = jnp.bfloat16
norm_floor = 0.0001


def bits_below(limit):
    found = []
    bit = limit // 2
    while bit:
        found.append(bit)
        bit //= 2
    return found


def low_bit(value):
    return value & -value


def rounds_of(seqs):
    found = []
    half = 2
    while half < seqs:
        found.append(half)
        half *= 2
    return found


def meet(peers):
    barrier = pltpu.get_barrier_semaphore()
    expected = 0
    for present, device in peers:
        if present is True:
            pl.semaphore_signal(barrier, inc=1, device_id=device, device_id_type=MESH)
            expected = expected + 1
        else:

            @pl.when(present)
            def _():
                pl.semaphore_signal(barrier, inc=1, device_id=device, device_id_type=MESH)

            expected = expected + present.astype(jnp.int32)
    pl.semaphore_wait(barrier, expected)


def remote(source, target, send_sem, recv_sem, device):
    return pltpu.make_async_remote_copy(
        src_ref=source,
        dst_ref=target,
        send_sem=send_sem,
        recv_sem=recv_sem,
        device_id=device,
        device_id_type=MESH,
    )


def dot(left, right, contract=((1,), (0,))):
    return lax.dot_general(
        left.astype(BF16), right.astype(BF16), (contract, ((), ())), preferred_element_type=F32
    )


def split(value):
    high = value.astype(BF16)
    return high, (value - high.astype(F32)).astype(BF16)


def dot3(left, right, contract=((1,), (0,))):
    lh, ll = left if isinstance(left, tuple) else split(left)
    rh, rl = right if isinstance(right, tuple) else split(right)
    axis = contract[1][0]
    both = dot(jnp.concatenate([lh, lh], axis=1), jnp.concatenate([rh, rl], axis=axis), contract)
    return both + dot(ll, rh, contract)


def layer_kernel(
    seqs, n, heads,
    x_ref, wq, wk, wv, wg, beta_in, step_in, taps_in, rates_in, bias_in, shift_in, gain_in, w_ref,
    out_ref,
    w_all, w_flat, spread, x_own, buf, beside, prior, raw, local, reader,
    slab_a, slab_c, mate_a, mate_c, go_a, go_c, in_a, in_c, pre_a, pre_c,
    w_buf, hid, acc,
    beta_ref, step_ref, taps, gain, rates, beta_bias, decay_bias,
    load_sem, small_sem, x_sem, t_send, t_recv, x_send, x_recv, p_send, p_recv, own_sem, w_send, w_recv,
    v_send, v_recv, sa_send, sa_recv, sc_send, sc_recv, side_send, a_send, a_recv, c_send, c_recv,
    h_send, h_recv,
):
    seq = lax.axis_index("seq")
    me = lax.axis_index("head")
    tokens, feats = x_ref.shape
    width = wq.shape[1]
    dim = LANES
    blocks = tokens // BLOCK
    columns = out_ref.shape[1]
    pieces = tokens // PIECE
    per_block = BLOCK // PIECE
    main = 2 * width + LANES
    total_width = w_all.shape[1]
    q_at = main
    g_at = main + width
    bits = bits_below(n)

    own_load = pltpu.make_async_copy(x_ref, x_own, x_sem)
    own_load.start()
    loads = []
    for w, at in ((wk, 0), (wv, width), (wq, q_at), (wg, g_at)):
        loads.append(pltpu.make_async_copy(w, w_all.at[:, pl.ds(at, width)], load_sem))
    smalls = [
        pltpu.make_async_copy(source, target, small_sem.at[i])
        for i, (source, target) in enumerate((
            (beta_in, beta_ref), (step_in, step_ref), (taps_in, taps), (gain_in, gain),
            (rates_in, rates), (bias_in, beta_bias), (shift_in, decay_bias),
        ))
    ]
    for load in smalls + loads:
        load.start()
    has_next = seq < seqs - 1
    has_before = seq > 0
    odd = seq % 2
    is_odd = odd == 1
    mate = seq + 1 - 2 * odd
    lone = heads // 2
    rounds = rounds_of(seqs)
    uppers, sources, origins, whole = [], [], [], []
    for half in rounds:
        inside = seq % (2 * half)
        uppers.append(inside >= half)
        sources.append(inside // 2 == half // 2 - 1)
        origins.append(seq - inside + half - 2 + odd)
        whole.append(seq - inside > 0)
    starts = seq == 1 if rounds else seq < 0
    gives_c = [seq >= 0 if h < lone else seq != 1 for h in range(heads)]
    gives_a = [seq != 0 if h < lone else seq >= 2 for h in range(heads)]
    takes_c = [seq >= 0 if h < lone else seq != 0 for h in range(heads)]
    takes_a = [seq != 1 if h < lone else seq >= 2 for h in range(heads)]
    peers = [(True, (seq, me ^ m)) for m in range(1, n)]
    peers += [(has_next, (seq + 1, me ^ m)) for m in range(2)]
    peers += [(has_before, (seq - 1, me ^ m)) for m in range(2)]
    for r, half in enumerate(rounds):
        peers += [(sources[r], (seq + 2 + 2 * j, me)) for j in range(half // 2)]
        peers += [(uppers[r], (origins[r], me))]
    meet(peers)
    own_load.wait()

    forwards = [m for m in range(1, n) if low_bit(m) > 1]
    lasts = [m for m in range(1, n) if low_bit(m) == 1]

    def slot_of(m, c):
        if m in forwards:
            return forwards.index(m) * pieces + c
        return len(forwards) * pieces + lasts.index(m) * blocks + c // per_block

    def hop(m, bit, c):
        piece = pl.ds(c * PIECE, PIECE)
        source = x_own.at[piece] if m == 0 else buf.at[m, piece]
        got = m | bit
        return remote(
            source, buf.at[got, piece], x_send.at[got - 1], x_recv.at[slot_of(got, c)],
            (seq, me ^ bit),
        )

    own_tail = x_own.at[pl.ds(tokens - PRIOR, PRIOR)]
    evens = list(range(2, n, 2))
    crossings = [
        remote(own_tail, beside.at[i], t_send.at[i], t_recv.at[i], (seq, me ^ m))
        for i, m in enumerate(evens)
    ]
    for crossing in crossings:
        crossing.start()

    def send_tail(source, m):
        @pl.when(has_next)
        def _():
            for bit in range(2):
                remote(
                    source, prior.at[m | bit], p_send, p_recv, (seq + 1, me ^ bit)
                ).start()

    send_tail(own_tail, 0)
    hops = {}
    for c in range(pieces):
        for bit in bits:
            hops[bit, c] = hop(0, bit, c)
            hops[bit, c].start()

    row = lax.broadcasted_iota(jnp.int32, (BLOCK, BLOCK), 0)
    col = lax.broadcasted_iota(jnp.int32, (BLOCK, BLOCK), 1)
    for j in range(BASE - 1):
        spread[:, pl.ds(j * LANES, LANES)] = (row == col // BASE * BASE + j).astype(F32).astype(BF16)

    for load in smalls:
        load.wait()
    w_flat[...] = jnp.zeros(w_flat.shape, F32)
    w_flat[pl.ds(0, heads), :] = beta_ref[...].astype(F32)
    w_flat[pl.ds(heads, heads), :] = step_ref[...].astype(F32)
    for i in range(w_flat.shape[1] // LANES):
        piece = pl.ds(i * LANES, LANES)
        w_all[piece, pl.ds(2 * width, LANES)] = w_flat[:, piece].T.astype(BF16)
    flat = w_all.at[:, pl.ds(0, len(loads) * width)]
    pltpu.make_async_copy(flat, flat, load_sem).wait()

    def weights_of(m, cols):
        start = pl.multiple_of((me ^ m) * feats, LANES)
        return w_all[pl.ds(start, feats), cols]

    def whole_block(m, b):
        return buf.at[m, pl.ds(b * BLOCK, BLOCK)]

    def arrive(m, b):
        if m in lasts:
            here = whole_block(m, b)
            remote(
                here, here, x_send.at[m - 1], x_recv.at[slot_of(m, b * per_block)], (seq, me ^ 1)
            ).wait_recv()
            return
        for c in range(b * per_block, (b + 1) * per_block):
            hops[m, c].wait_recv()
            for bit in bits:
                if bit < low_bit(m):
                    hops[m | bit, c] = hop(m, bit, c)
                    hops[m | bit, c].start()

    every = pl.ds(0, total_width)
    first_cols = pl.ds(0, main)
    rest_cols = pl.ds(main, total_width - main)

    def add(ms, at, count, cols):
        here = pl.ds(PRIOR + at, count)
        total = None
        for m in ms:
            values = x_own[pl.ds(at, count), :] if m == 0 else buf[m, pl.ds(at, count), :]
            term = jnp.dot(values, weights_of(m, cols), preferred_element_type=F32)
            total = term if total is None else total + term
        if 0 not in ms:
            total = total + raw[here, cols]
        raw[here, cols] = total

    near = [m for m in range(1, n) if m == 1]
    far = sorted(range(2, n), key=lambda m: (-low_bit(m), m))
    step = 2 * BLOCK if tokens % (2 * BLOCK) == 0 else BLOCK
    for at in range(0, tokens, step):
        add([0], at, step, every)

    for i, m in enumerate(evens):
        crossings[i].wait_recv()
        send_tail(beside.at[i], m)

    for at in range(0, tokens, step):
        for m in near:
            for b in range(at // BLOCK, (at + step) // BLOCK):
                arrive(m, b)
            add([m], at, step, every)

    within = row >= col
    before = row > col
    eye = (row == col).astype(F32)
    lower = within.astype(F32).astype(BF16)
    lower3 = jnp.concatenate([lower, lower, lower], axis=1)
    lane = lax.broadcasted_iota(jnp.int32, (1, LANES), 1)
    offset = jnp.zeros((1, LANES), F32)
    rate = jnp.zeros((1, LANES), F32)
    for h in range(heads):
        offset = jnp.where(lane == h, beta_bias[h], offset)
        offset = jnp.where(lane == heads + h, decay_bias[h], offset)
        rate = jnp.where(lane == heads + h, rates[h], rate)
    rate = -jnp.exp(rate)
    tiles = BLOCK // BASE
    tile_shape = (tiles, BASE, BLOCK)
    on_tile = (
        lax.broadcasted_iota(jnp.int32, tile_shape, 0)
        == lax.broadcasted_iota(jnp.int32, tile_shape, 2) // BASE
    )
    small_eye = (
        lax.broadcasted_iota(jnp.int32, (BASE, BLOCK), 0)
        == lax.broadcasted_iota(jnp.int32, (BASE, BLOCK), 1) % BASE
    ).astype(F32)

    def add_prior():
        @pl.when(has_before)
        def _():
            total = jnp.zeros((PRIOR, total_width), F32)
            remote(prior, prior, p_send, p_recv, (seq - 1, me)).wait_recv()
            for m in range(n):
                total = total + jnp.dot(prior[m], weights_of(m, every), preferred_element_type=F32)
            raw[pl.ds(0, PRIOR), :] = total

        @pl.when(jnp.logical_not(has_before))
        def _():
            raw[pl.ds(0, PRIOR), :] = jnp.zeros((PRIOR, total_width), F32)

    def mixed(kind, h, b):
        base = (q_at, 0, width)[kind] + h * dim
        start = PRIOR + b * BLOCK
        total = None
        for s in range(taps.shape[1]):
            tap = taps[kind, pl.ds(s, 1), pl.ds(h * dim, dim)]
            term = tap * raw[pl.ds(start - s, BLOCK), pl.ds(base, dim)]
            total = term if total is None else total + term
        return total * jax.nn.sigmoid(total)

    def unit(values):
        return values * lax.rsqrt(jnp.sum(values * values, axis=-1, keepdims=True) + 1.0)

    def bases(lows):
        stack = []
        for low in lows:
            packed = jnp.sum(jnp.where(on_tile, low.reshape(tile_shape), 0.0), axis=0)
            high = packed.astype(BF16).astype(F32)
            stack += [high, packed - high]
        found = dot(jnp.concatenate(stack, axis=0), spread[...])
        results = []
        for h in range(len(lows)):
            inverse = small_eye
            for j in range(BASE - 1):
                cols = slice(j * LANES, (j + 1) * LANES)
                at = 2 * BASE * h
                factor = found[at : at + BASE, cols] + found[at + BASE : at + 2 * BASE, cols]
                inverse = inverse - factor * inverse[j : j + 1, :]
            results.append(
                jnp.where(on_tile, inverse[None], 0.0).reshape(BLOCK, BLOCK)
            )
        return results

    def small_terms(b):
        small = raw[pl.ds(PRIOR + b * BLOCK, BLOCK), pl.ds(2 * width, LANES)] + offset
        betas = jax.nn.sigmoid(small)
        steps = rate * (jnp.maximum(small, 0.0) + jnp.log1p(jnp.exp(-jnp.abs(small))))
        one, rest = split(steps)
        left = steps - one.astype(F32) - rest.astype(F32)
        run = dot(lower3, jnp.concatenate([one, rest, left.astype(BF16)], axis=0))
        return betas, run, run.T

    def block_terms(b, before_slab, midway):
        betas, run, across = small_terms(b)
        keys, decays, growths, lows, weighteds, ends = [], [], [], [], [], []
        sides = []
        for h in range(heads):
            k = unit(mixed(1, h, b))
            down = run[:, heads + h : heads + h + 1]
            along = across[heads + h : heads + h + 1, :]
            beta = betas[:, h : h + 1]
            last = down[BLOCK - 1 : BLOCK, :]
            decay = jnp.where(within, jnp.exp(jnp.minimum(down - along, 0.0)), 0.0)
            key = split(k)
            gram = dot3(key, key, ((1,), (1,)))
            lows.append(jnp.where(before, beta * decay * gram, 0.0))
            keys.append(key)
            decays.append(decay)
            growth = jnp.exp(down)
            growths.append(growth)
            ends.append(jnp.exp(last))
            weighteds.append((jnp.exp(last - down) * k).T)
        inverses = bases(lows)
        for h in range(heads):
            beta = betas[:, h : h + 1]
            v = mixed(2, h, b)
            scale = beta * growths[h]
            if before_slab is None:
                k = keys[h][0].astype(F32) + keys[h][1].astype(F32)
                sides.append(jnp.concatenate([-scale * k, beta * v], axis=1))
            else:
                moved = -scale * dot3(keys[h], before_slab[h])
                sides.append(
                    jnp.concatenate([moved[:, :dim], moved[:, dim:] + beta * v], axis=1)
                )
        span = BASE
        while 4 * span < BLOCK:
            area = (row // (4 * span) == col // (4 * span)) & (row // span > col // span)
            shares = [split(inv) for inv in inverses]
            links = [
                split(dot3(share, jnp.where(area, low, 0.0))) for share, low in zip(shares, lows)
            ]
            nexts = []
            for inv, share, link in zip(inverses, shares, links):
                pair = dot3(link, tuple(
                    jnp.concatenate([a, c], axis=1) for a, c in zip(share, link)
                ))
                nexts.append((inv - pair[:, :BLOCK], pair[:, BLOCK:]))
            inverses = [z + dot3(square, z) for z, square in nexts]
            span *= 4
        midway()
        area = row // span > col // span
        wide = [
            dot3(inv, jnp.concatenate([jnp.where(area, low, 0.0), side], axis=1))
            for inv, low, side in zip(inverses, lows, sides)
        ]
        links = [split(got[:, :BLOCK]) for got in wide]
        solved = [got[:, BLOCK:] for got in wide]
        level = span
        while level < BLOCK:
            nexts = []
            for link, have in zip(links, solved):
                share = split(have)
                more = level * 2 < BLOCK
                right = tuple(
                    jnp.concatenate([a, c], axis=1) for a, c in zip(share, link)
                ) if more else share
                got = dot3(link, right)
                nexts.append((got[:, : 2 * dim], got[:, 2 * dim :] if more else None))
            sign = -1.0 if level == span else 1.0
            solved = [have + sign * got for have, (got, _) in zip(solved, nexts)]
            links = [split(square) if square is not None else None for _, square in nexts]
            level *= 2
        slabs = []
        shares = [split(have) for have in solved]
        for h in range(heads):
            got = dot3(weighteds[h], shares[h])
            if before_slab is None:
                slabs.append(jnp.concatenate([ends[h] * eye + got[:, :dim], got[:, dim:]], axis=1))
            else:
                high, rest = before_slab[h]
                have = high.astype(F32) + rest.astype(F32)
                slabs.append(ends[h] * have + got)

        def outputs():
            for h in range(heads):
                q = unit(mixed(0, h, b))
                mix = decays[h] * dot3(q, keys[h], ((1,), (1,)))
                lead = growths[h] * q
                if before_slab is None:
                    got = dot3(mix, shares[h])
                    read, here = got[:, :dim] + lead, got[:, dim:]
                else:
                    right = tuple(
                        jnp.concatenate([a, c], axis=0)
                        for a, c in zip(shares[h], before_slab[h])
                    )
                    got = dot3(jnp.concatenate([mix, lead], axis=1), right)
                    read, here = got[:, :dim], got[:, dim:]
                reader[h, b] = read.astype(BF16)
                local[h, b] = here

        return slabs, outputs

    def columns_of(m):
        return pl.ds(pl.multiple_of((me ^ m) * columns, LANES), columns)

    own = pltpu.make_async_copy(w_ref.at[:, columns_of(0)], w_buf.at[0], own_sem)
    share = width // 2

    def part_of(which):
        return pl.ds(pl.multiple_of(which * share, share), share)

    moves, passes = {}, {}
    for m in range(1, n):
        if m in near:
            source, target = w_ref.at[:, columns_of(m)], w_buf.at[m]
        else:
            source, target = w_ref.at[part_of(odd), columns_of(m)], w_buf.at[m, part_of(odd)]
            passes[m] = remote(
                w_buf.at[m, part_of(odd)], w_buf.at[m, part_of(odd)], v_send, v_recv, (mate, me)
            )
        moves[m] = remote(
            source, target, w_send, w_recv.at[0 if m in near else 1], (seq, me ^ m)
        )
    half_slots = w_buf.at[pl.ds(0, len(passes) // 2)]
    all_halves = remote(half_slots, half_slots, v_send, v_recv, (mate, me))
    far_halves = remote(half_slots, half_slots, w_send, w_recv.at[1], (seq, me ^ n // 2))
    all_slots = w_buf.at[pl.ds(0, len(passes) // 2 + len(near))]
    all_moves = remote(all_slots, all_slots, w_send, w_recv.at[0], (seq, me ^ 1))

    def arrive_block(b):
        for m in far:
            if low_bit(m) > 1:
                arrive(m, b)

    direct = [m for m in far if low_bit(m) > 1]
    passed = [m for m in far if low_bit(m) == 1]
    slabs = None
    outputs = []
    add_prior()
    arrive_block(0)
    add(direct, 0, BLOCK, first_cols)
    for b in range(blocks):
        for m in passed:
            arrive(m, b)
        add(passed, b * BLOCK, BLOCK, first_cols)

        def midway():
            if b + 1 < blocks:
                arrive_block(b + 1)
                add(direct, (b + 1) * BLOCK, BLOCK, first_cols)
            if b + 2 == max(blocks, 2):
                own.start()
                for m in far + near:
                    moves[m].start()

        prior_slab = None if slabs is None else [split(value) for value in slabs]
        slabs, later = block_terms(b, prior_slab, midway)
        outputs.append(later)

    swaps_a, swaps_c = [], []
    for h in range(heads):
        slab_c[h] = slabs[h][:, dim:].astype(slab_c.dtype)
        slab_a[h] = slabs[h][:, :dim].astype(slab_a.dtype)
        swaps_a.append(
            remote(slab_a.at[h], mate_a.at[h], sa_send.at[h], sa_recv.at[h], (mate, me))
        )
        swaps_c.append(
            remote(slab_c.at[h], mate_c.at[h], sc_send.at[h], sc_recv.at[h], (mate, me))
        )
    for h in range(heads):

        @pl.when(gives_c[h])
        def _():
            swaps_c[h].start()

        @pl.when(gives_a[h])
        def _():
            swaps_a[h].start()

    blank = jnp.zeros((dim, dim), slab_a.dtype)
    for h in range(heads):

        @pl.when(jnp.logical_not(takes_a[h]))
        def _():
            mate_a[h] = blank

        @pl.when(jnp.logical_not(takes_c[h]))
        def _():
            mate_c[h] = blank
        pre_c[h] = jnp.zeros((dim, dim), F32)

    for at in range(0, tokens, step):
        add(far, at, step, rest_cols)
    for h in range(heads):
        place = pl.ds(PRIOR, tokens), pl.ds(g_at + h * dim, dim)
        gate = raw[place]
        raw[place] = gain[...] * (gate * jax.nn.sigmoid(gate))
    for later in outputs:
        later()

    def total_copy(source, target, send_sem, recv_sem, r, h, j):
        return remote(
            source.at[r, h], target.at[r, h], send_sem.at[rounds[r] // 2 - 1 + j, h],
            recv_sem.at[r, h], (seq + 2 + 2 * j, me),
        )

    totals_c, totals_a = {}, {}
    for r, half in enumerate(rounds):
        for h in range(heads):
            for j in range(half // 2):
                totals_c[r, h, j] = total_copy(go_c, in_c, c_send, c_recv, r, h, j)
                if r + 1 < len(rounds):
                    totals_a[r, h, j] = total_copy(go_a, in_a, a_send, a_recv, r, h, j)
    asides = {
        h: remote(go_c.at[0, h], in_c.at[0, h], side_send.at[h - lone], c_recv.at[0, h], (seq + 1, me))
        for h in range(lone, heads) if rounds
    }
    pair_a, pair_c, firsts = [], [], []

    def giver(r, h):
        return sources[r] & (seq != 0) if r == 0 and h >= lone else sources[r]

    def send_total(r, h):
        @pl.when(giver(r, h))
        def _():
            total = pair_c[h] if r == 0 else dot(pair_a[h], pre_c[h]) + pair_c[h]
            go_c[r, h] = total.astype(go_c.dtype)
            for j in reversed(range(rounds[r] // 2)):
                totals_c[r, h, j].start()

            if r + 1 == len(rounds):
                return

            @pl.when(whole[r])
            def _():
                total = pair_a[h] if r == 0 else dot(pair_a[h], pre_a[h])
                go_a[r, h] = total.astype(go_a.dtype)
                for j in reversed(range(rounds[r] // 2)):
                    totals_a[r, h, j].start()

        if r == 0 and h in asides:

            @pl.when(starts)
            def _():
                asides[h].start()

    def take_total(r, h):
        first = seq % rounds[r] < 2

        @pl.when(uppers[r])
        def _():
            totals_c[r, h, 0].wait_recv()

            @pl.when(first)
            def _():
                pre_c[h] = in_c[r, h].astype(F32)

            @pl.when(jnp.logical_not(first))
            def _():
                pre_c[h] = dot(pre_a[h], in_c[r, h]) + pre_c[h]

            if r + 1 == len(rounds):
                return

            @pl.when(whole[r])
            def _():
                totals_a[r, h, 0].wait_recv()

                @pl.when(first)
                def _():
                    pre_a[h] = in_a[r, h].astype(F32)

                @pl.when(jnp.logical_not(first))
                def _():
                    pre_a[h] = dot(pre_a[h], in_a[r, h])

    def hand_over():
        far_halves.wait_recv()
        for m in passes:
            passes[m].start()

    lifts = {}

    def lift_slot(m, h, b):
        if m in forwards:
            return (forwards.index(m) * blocks + b) * heads + h
        return (len(forwards) * heads + lasts.index(m)) * blocks + b

    def lift(m, bit, h, b):
        got = m | bit
        return remote(
            hid.at[m, b, h], hid.at[got, b, h],
            h_send.at[got - 1], h_recv.at[lift_slot(got, h, b)], (seq, me ^ bit),
        )

    def forward(m, h, b):
        limit = n if m == 0 else low_bit(m)
        for bit in bits:
            if bit < limit:
                lifts[m | bit, h, b] = lift(m, bit, h, b)
                lifts[m | bit, h, b].start()

    states = []

    def read(h, b):
        head_out = dot(reader[h, b], states[h]) + local[h, b]
        gate = raw[pl.ds(PRIOR + b * BLOCK, BLOCK), pl.ds(g_at + h * dim, dim)]
        scaled = head_out * lax.rsqrt(
            jnp.mean(head_out * head_out, axis=-1, keepdims=True) + norm_floor
        )
        hid[0, b, h] = (scaled * gate).astype(BF16)
        forward(0, h, b)

    upper = uppers[-1] if rounds else seq < 0

    def relay(h):
        for r in range(len(rounds) - 1):
            take_total(r, h)
            send_total(r + 1, h)

    for h in range(heads):
        @pl.when(takes_c[h])
        def _():
            swaps_c[h].wait_recv()

        @pl.when(takes_a[h])
        def _():
            swaps_a[h].wait_recv()

        here_a, here_c = slab_a[h].astype(F32), slab_c[h].astype(F32)
        there_a, there_c = mate_a[h].astype(F32), mate_c[h].astype(F32)
        left = jnp.where(is_odd, here_a, there_a)
        right_a = jnp.where(is_odd, there_a, here_a)
        right_c = jnp.where(is_odd, there_c, here_c)
        back_c = jnp.where(is_odd, here_c, there_c)
        moved = dot(left, jnp.concatenate([right_a, right_c], axis=1))
        pair_a.append(moved[:, :dim])
        pair_c.append(moved[:, dim:] + back_c)
        firsts.append((right_a, right_c))
        if rounds:
            send_total(0, h)

        @pl.when(jnp.logical_not(upper))
        def _():
            relay(h)


    hand_over()

    for h in range(heads):
        @pl.when(upper)
        def _():
            relay(h)

        if rounds:
            take_total(len(rounds) - 1, h)
        first_a, first_c = firsts[h]
        state = pre_c[h]
        states.append(jnp.where(is_odd, dot(first_a, state) + first_c, state))
        for b in range(blocks):
            read(h, b)

    own.wait()
    for m in near:
        moves[m].wait_recv()

    def rows_of(m, b):
        return jnp.concatenate([hid[m, b, h] for h in range(heads)], axis=1)

    def settle(m, b):
        here = hid.at[m, b]
        remote(
            here, here, h_send.at[m - 1], h_recv.at[lift_slot(m, 0, b)], (seq, me ^ 1)
        ).wait_recv()

    for h in range(heads):
        for b in range(blocks):
            for m in forwards:
                lifts[m, h, b].wait_recv()
                forward(m, h, b)
            if h + 1 == heads:
                total = jnp.dot(rows_of(0, b), w_buf[0], preferred_element_type=F32)
                for m in near:
                    settle(m, b)
                    total = total + jnp.dot(rows_of(m, b), w_buf[m], preferred_element_type=F32)
                acc[b] = total
    all_halves.wait_recv()
    for b in range(blocks):
        total = acc[b]
        for m in far:
            if m in lasts:
                settle(m, b)
            total = total + jnp.dot(rows_of(m, b), w_buf[m], preferred_element_type=F32)
        out_ref[pl.ds(b * BLOCK, BLOCK), :] = total.astype(BF16)

    for m in range(1, n):
        remote(buf.at[m], buf.at[m], x_send.at[m - 1], x_recv.at[0], (seq, me ^ 1)).wait_send()
        remote(hid.at[m], hid.at[m], h_send.at[m - 1], h_recv.at[0], (seq, me ^ 1)).wait_send()
    for crossing in crossings:
        crossing.wait_send()
    all_moves.wait_send()
    all_halves.wait_send()

    for h in range(heads):

        @pl.when(gives_c[h])
        def _():
            swaps_c[h].wait_send()

        @pl.when(gives_a[h])
        def _():
            swaps_a[h].wait_send()

        if h in asides:

            @pl.when(starts)
            def _():
                asides[h].wait_send()

        for r, half in enumerate(rounds):

            @pl.when(giver(r, h))
            def _():
                for j in range(half // 2):
                    totals_c[r, h, j].wait_send()

                if r + 1 == len(rounds):
                    return

                @pl.when(whole[r])
                def _():
                    for j in range(half // 2):
                        totals_a[r, h, j].wait_send()

    @pl.when(has_next)
    def _():
        remote(prior, prior, p_send, p_recv, (seq + 1, me)).wait_send()


def on_device(
    seqs, n,
    layer_in, query_weight, key_weight, value_weight, gate_weight, beta_weight, decay_weight,
    conv_weight, decay_log, beta_bias, decay_bias, norm_gain, out_weight,
):
    tokens, feats = layer_in.shape
    model, width = query_weight.shape
    heads = beta_weight.shape[1]
    dim = width // heads
    blocks = tokens // BLOCK
    per_block = BLOCK // PIECE
    ways = (n // 2 - 1) * blocks
    total_width = 4 * width + LANES
    columns = out_weight.shape[1] // n
    vmem = pl.BlockSpec(memory_space=pltpu.VMEM)
    anywhere = pl.BlockSpec(memory_space=pl.ANY)
    dma = pltpu.SemaphoreType.DMA
    wire = BF16 if seqs <= 8 else F32
    steps = max(1, len(rounds_of(seqs)))
    most = max(1, seqs // 4)
    square = pltpu.VMEM((heads, dim, dim), wire)
    stage = pltpu.VMEM((steps, heads, dim, dim), wire)
    total = pltpu.VMEM((heads, dim, dim), F32)
    return pl.pallas_call(
        functools.partial(layer_kernel, seqs, n, heads),
        out_shape=pltpu.VMEM((tokens, columns), BF16),
        in_specs=[anywhere] * 13,
        out_specs=vmem,
        scratch_shapes=[
            pltpu.VMEM((model, total_width), BF16),
            pltpu.VMEM((LANES, model), F32),
            pltpu.VMEM((LANES, (BASE - 1) * LANES), BF16),
            pltpu.VMEM((tokens, feats), BF16),
            pltpu.VMEM((n, tokens, feats), BF16),
            pltpu.VMEM((n // 2 - 1, PRIOR, feats), BF16),
            pltpu.VMEM((n, PRIOR, feats), BF16),
            pltpu.VMEM((PRIOR + tokens, total_width), F32),
            pltpu.VMEM((heads, blocks, BLOCK, dim), F32),
            pltpu.VMEM((heads, blocks, BLOCK, dim), BF16),
            square, square, square, square,
            stage, stage, stage, stage,
            total, total,
            pltpu.VMEM((n, width, columns), BF16),
            pltpu.VMEM((n, blocks, heads, BLOCK, dim), BF16),
            pltpu.VMEM((blocks, BLOCK, columns), F32),
            pltpu.VMEM((heads, model), BF16),
            pltpu.VMEM((heads, model), BF16),
            pltpu.VMEM((conv_weight.shape[1], conv_weight.shape[0], width), F32),
            pltpu.VMEM((1, dim), F32),
            pltpu.SMEM((heads,), F32),
            pltpu.SMEM((heads,), F32),
            pltpu.SMEM((heads,), F32),
            dma(()),
            dma((7,)),
            dma(()),
            dma((n // 2 - 1,)),
            dma((n // 2 - 1,)),
            dma((n - 1,)),
            dma((ways * per_block + n // 2 * blocks,)),
            dma(()),
            dma(()),
            dma(()),
            dma(()),
            dma((2,)),
            dma(()),
            dma(()),
            dma((heads,)),
            dma((heads,)),
            dma((heads,)),
            dma((heads,)),
            dma((heads - heads // 2,)),
            dma((max(1, seqs // 4 - 1), heads)),
            dma((max(1, steps - 1), heads)),
            dma((max(1, seqs // 2 - 1), heads)),
            dma((steps, heads)),
            dma((n - 1,)),
            dma((ways * heads + n // 2 * blocks,)),
        ],
        compiler_params=pltpu.CompilerParams(
            collective_id=0, has_side_effects=True, vmem_limit_bytes=60 * 1024 * 1024
        ),
    )(
        layer_in, query_weight, key_weight, value_weight, gate_weight,
        beta_weight.T, decay_weight.T, conv_weight.transpose(1, 0, 2),
        decay_log, beta_bias, decay_bias, norm_gain[None], out_weight,
    )


def solution(mesh):
    return jax.shard_map(
        functools.partial(on_device, mesh.shape["seq"], mesh.shape["head"]),
        mesh=mesh,
        in_specs=(
            P("seq", "head"),
            P(None, "head"),
            P(None, "head"),
            P(None, "head"),
            P(None, "head"),
            P(None, "head"),
            P(None, "head"),
            P(None, None, "head"),
            P("head"),
            P("head"),
            P("head"),
            P(),
            P("head", None),
        ),
        out_specs=P("seq", "head"),
        check_vma=False,
    )
```

```python
import functools

import jax
import jax.numpy as jnp
from jax import lax
from jax.experimental import pallas as pl
from jax.experimental.pallas import tpu as pltpu
from jax.sharding import PartitionSpec as P

BLOCK = 128
PRIOR = 8
LANES = 128
PIECE = 128
BASE = 8

LAG = 2
MESH = pl.DeviceIdType.MESH
F32 = jnp.float32
BF16 = jnp.bfloat16
norm_floor = 0.0001


def bits_below(limit):
    found = []
    bit = limit // 2
    while bit:
        found.append(bit)
        bit //= 2
    return found


def low_bit(value):
    return value & -value


def rounds_of(seqs):
    found = []
    half = 2
    while half < seqs:
        found.append(half)
        half *= 2
    return found


def meet(peers):
    barrier = pltpu.get_barrier_semaphore()
    expected = 0
    for present, device in peers:
        if present is True:
            pl.semaphore_signal(barrier, inc=1, device_id=device, device_id_type=MESH)
            expected = expected + 1
        else:

            @pl.when(present)
            def _():
                pl.semaphore_signal(barrier, inc=1, device_id=device, device_id_type=MESH)

            expected = expected + present.astype(jnp.int32)
    pl.semaphore_wait(barrier, expected)


def remote(source, target, send_sem, recv_sem, device):
    return pltpu.make_async_remote_copy(
        src_ref=source,
        dst_ref=target,
        send_sem=send_sem,
        recv_sem=recv_sem,
        device_id=device,
        device_id_type=MESH,
    )


def dot(left, right, contract=((1,), (0,))):
    return lax.dot_general(
        left.astype(BF16), right.astype(BF16), (contract, ((), ())), preferred_element_type=F32
    )


def split(value):
    high = value.astype(BF16)
    return high, (value - high.astype(F32)).astype(BF16)


def dot3(left, right, contract=((1,), (0,))):
    lh, ll = left if isinstance(left, tuple) else split(left)
    rh, rl = right if isinstance(right, tuple) else split(right)
    axis = contract[1][0]
    both = dot(jnp.concatenate([lh, lh], axis=1), jnp.concatenate([rh, rl], axis=axis), contract)
    return both + dot(ll, rh, contract)


def layer_kernel(
    seqs, n, heads,
    x_ref, wq, wk, wv, wg, beta_in, step_in, taps_in, rates_in, bias_in, shift_in, gain_in, w_ref,
    out_ref,
    w_all, w_flat, spread, x_own, buf, beside, prior, raw, local, reader,
    slab_a, slab_c, mate_a, mate_c, go_a, go_c, in_a, in_c, pre_a, pre_c,
    w_buf, hid, acc,
    beta_ref, step_ref, taps, gain, rates, beta_bias, decay_bias,
    load_sem, small_sem, x_sem, t_send, t_recv, x_send, x_recv, p_send, p_recv, own_sem, w_send, w_recv,
    v_send, v_recv, sa_send, sa_recv, sc_send, sc_recv, side_send, a_send, a_recv, c_send, c_recv,
    h_send, h_recv,
):
    seq = lax.axis_index("seq")
    me = lax.axis_index("head")
    tokens, feats = x_ref.shape
    width = wq.shape[1]
    dim = LANES
    blocks = tokens // BLOCK
    columns = out_ref.shape[1]
    pieces = tokens // PIECE
    per_block = BLOCK // PIECE
    main = 2 * width + LANES
    total_width = w_all.shape[1]
    q_at = main
    g_at = main + width
    bits = bits_below(n)

    own_load = pltpu.make_async_copy(x_ref, x_own, x_sem)
    own_load.start()
    loads = []
    for w, at in ((wk, 0), (wv, width), (wq, q_at), (wg, g_at)):
        loads.append(pltpu.make_async_copy(w, w_all.at[:, pl.ds(at, width)], load_sem))
    smalls = [
        pltpu.make_async_copy(source, target, small_sem.at[i])
        for i, (source, target) in enumerate((
            (beta_in, beta_ref), (step_in, step_ref), (taps_in, taps), (gain_in, gain),
            (rates_in, rates), (bias_in, beta_bias), (shift_in, decay_bias),
        ))
    ]
    for load in smalls + loads:
        load.start()
    has_next = seq < seqs - 1
    has_before = seq > 0
    odd = seq % 2
    is_odd = odd == 1
    mate = seq + 1 - 2 * odd
    lone = heads // 2
    rounds = rounds_of(seqs)
    uppers, sources, origins, whole = [], [], [], []
    for half in rounds:
        inside = seq % (2 * half)
        uppers.append(inside >= half)
        sources.append(inside // 2 == half // 2 - 1)
        origins.append(seq - inside + half - 2 + odd)
        whole.append(seq - inside > 0)
    starts = seq == 1 if rounds else seq < 0
    gives_c = [seq >= 0 if h < lone else seq != 1 for h in range(heads)]
    gives_a = [seq != 0 if h < lone else seq >= 2 for h in range(heads)]
    takes_c = [seq >= 0 if h < lone else seq != 0 for h in range(heads)]
    takes_a = [seq != 1 if h < lone else seq >= 2 for h in range(heads)]
    peers = [(True, (seq, me ^ m)) for m in range(1, n)]
    peers += [(has_next, (seq + 1, me ^ m)) for m in range(2)]
    peers += [(has_before, (seq - 1, me ^ m)) for m in range(2)]
    for r, half in enumerate(rounds):
        peers += [(sources[r], (seq + 2 + 2 * j, me)) for j in range(half // 2)]
        peers += [(uppers[r], (origins[r], me))]
    meet(peers)
    own_load.wait()

    forwards = [m for m in range(1, n) if low_bit(m) > 1]
    lasts = [m for m in range(1, n) if low_bit(m) == 1]

    def slot_of(m, c):
        if m in forwards:
            return forwards.index(m) * pieces + c
        return len(forwards) * pieces + lasts.index(m) * blocks + c // per_block

    def hop(m, bit, c):
        piece = pl.ds(c * PIECE, PIECE)
        source = x_own.at[piece] if m == 0 else buf.at[m, piece]
        got = m | bit
        return remote(
            source, buf.at[got, piece], x_send.at[got - 1], x_recv.at[slot_of(got, c)],
            (seq, me ^ bit),
        )

    own_tail = x_own.at[pl.ds(tokens - PRIOR, PRIOR)]
    evens = list(range(2, n, 2))
    crossings = [
        remote(own_tail, beside.at[i], t_send.at[i], t_recv.at[i], (seq, me ^ m))
        for i, m in enumerate(evens)
    ]
    for crossing in crossings:
        crossing.start()

    def send_tail(source, m):
        @pl.when(has_next)
        def _():
            for bit in range(2):
                remote(
                    source, prior.at[m | bit], p_send, p_recv, (seq + 1, me ^ bit)
                ).start()

    send_tail(own_tail, 0)
    hops = {}
    for c in range(pieces):
        for bit in bits:
            hops[bit, c] = hop(0, bit, c)
            hops[bit, c].start()

    row = lax.broadcasted_iota(jnp.int32, (BLOCK, BLOCK), 0)
    col = lax.broadcasted_iota(jnp.int32, (BLOCK, BLOCK), 1)
    for j in range(BASE - 1):
        spread[:, pl.ds(j * LANES, LANES)] = (row == col // BASE * BASE + j).astype(F32).astype(BF16)

    for load in smalls:
        load.wait()
    w_flat[...] = jnp.zeros(w_flat.shape, F32)
    w_flat[pl.ds(0, heads), :] = beta_ref[...].astype(F32)
    w_flat[pl.ds(heads, heads), :] = step_ref[...].astype(F32)
    for i in range(w_flat.shape[1] // LANES):
        piece = pl.ds(i * LANES, LANES)
        w_all[piece, pl.ds(2 * width, LANES)] = w_flat[:, piece].T.astype(BF16)
    flat = w_all.at[:, pl.ds(0, len(loads) * width)]
    pltpu.make_async_copy(flat, flat, load_sem).wait()

    def weights_of(m, cols):
        start = pl.multiple_of((me ^ m) * feats, LANES)
        return w_all[pl.ds(start, feats), cols]

    def whole_block(m, b):
        return buf.at[m, pl.ds(b * BLOCK, BLOCK)]

    def arrive(m, b):
        if m in lasts:
            here = whole_block(m, b)
            remote(
                here, here, x_send.at[m - 1], x_recv.at[slot_of(m, b * per_block)], (seq, me ^ 1)
            ).wait_recv()
            return
        for c in range(b * per_block, (b + 1) * per_block):
            hops[m, c].wait_recv()
            for bit in bits:
                if bit < low_bit(m):
                    hops[m | bit, c] = hop(m, bit, c)
                    hops[m | bit, c].start()

    every = pl.ds(0, total_width)
    first_cols = pl.ds(0, main)
    rest_cols = pl.ds(main, total_width - main)

    def add(ms, at, count, cols):
        here = pl.ds(PRIOR + at, count)
        total = None
        for m in ms:
            values = x_own[pl.ds(at, count), :] if m == 0 else buf[m, pl.ds(at, count), :]
            term = jnp.dot(values, weights_of(m, cols), preferred_element_type=F32)
            total = term if total is None else total + term
        if 0 not in ms:
            total = total + raw[here, cols]
        raw[here, cols] = total

    near = [m for m in range(1, n) if m == 1]
    far = sorted(range(2, n), key=lambda m: (-low_bit(m), m))
    step = 2 * BLOCK if tokens % (2 * BLOCK) == 0 else BLOCK
    for at in range(0, tokens, step):
        add([0], at, step, every)

    for i, m in enumerate(evens):
        crossings[i].wait_recv()
        send_tail(beside.at[i], m)

    for at in range(0, tokens, step):
        for m in near:
            for b in range(at // BLOCK, (at + step) // BLOCK):
                arrive(m, b)
            add([m], at, step, every)

    within = row >= col
    before = row > col
    eye = (row == col).astype(F32)
    lower = within.astype(F32).astype(BF16)
    lower3 = jnp.concatenate([lower, lower, lower], axis=1)
    lane = lax.broadcasted_iota(jnp.int32, (1, LANES), 1)
    offset = jnp.zeros((1, LANES), F32)
    rate = jnp.zeros((1, LANES), F32)
    for h in range(heads):
        offset = jnp.where(lane == h, beta_bias[h], offset)
        offset = jnp.where(lane == heads + h, decay_bias[h], offset)
        rate = jnp.where(lane == heads + h, rates[h], rate)
    rate = -jnp.exp(rate)
    tiles = BLOCK // BASE
    tile_shape = (tiles, BASE, BLOCK)
    on_tile = (
        lax.broadcasted_iota(jnp.int32, tile_shape, 0)
        == lax.broadcasted_iota(jnp.int32, tile_shape, 2) // BASE
    )
    small_eye = (
        lax.broadcasted_iota(jnp.int32, (BASE, BLOCK), 0)
        == lax.broadcasted_iota(jnp.int32, (BASE, BLOCK), 1) % BASE
    ).astype(F32)

    def add_prior():
        @pl.when(has_before)
        def _():
            total = jnp.zeros((PRIOR, total_width), F32)
            remote(prior, prior, p_send, p_recv, (seq - 1, me)).wait_recv()
            for m in range(n):
                total = total + jnp.dot(prior[m], weights_of(m, every), preferred_element_type=F32)
            raw[pl.ds(0, PRIOR), :] = total

        @pl.when(jnp.logical_not(has_before))
        def _():
            raw[pl.ds(0, PRIOR), :] = jnp.zeros((PRIOR, total_width), F32)

    def mixed(kind, h, b):
        base = (q_at, 0, width)[kind] + h * dim
        start = PRIOR + b * BLOCK
        total = None
        for s in range(taps.shape[1]):
            tap = taps[kind, pl.ds(s, 1), pl.ds(h * dim, dim)]
            term = tap * raw[pl.ds(start - s, BLOCK), pl.ds(base, dim)]
            total = term if total is None else total + term
        return total * jax.nn.sigmoid(total)

    def unit(values):
        return values * lax.rsqrt(jnp.sum(values * values, axis=-1, keepdims=True) + 1.0)

    def bases(lows):
        stack = []
        for low in lows:
            packed = jnp.sum(jnp.where(on_tile, low.reshape(tile_shape), 0.0), axis=0)
            high = packed.astype(BF16).astype(F32)
            stack += [high, packed - high]
        found = dot(jnp.concatenate(stack, axis=0), spread[...])
        results = []
        for h in range(len(lows)):
            inverse = small_eye
            for j in range(BASE - 1):
                cols = slice(j * LANES, (j + 1) * LANES)
                at = 2 * BASE * h
                factor = found[at : at + BASE, cols] + found[at + BASE : at + 2 * BASE, cols]
                inverse = inverse - factor * inverse[j : j + 1, :]
            results.append(
                jnp.where(on_tile, inverse[None], 0.0).reshape(BLOCK, BLOCK)
            )
        return results

    def small_terms(b):
        small = raw[pl.ds(PRIOR + b * BLOCK, BLOCK), pl.ds(2 * width, LANES)] + offset
        betas = jax.nn.sigmoid(small)
        steps = rate * (jnp.maximum(small, 0.0) + jnp.log1p(jnp.exp(-jnp.abs(small))))
        one, rest = split(steps)
        left = steps - one.astype(F32) - rest.astype(F32)
        run = dot(lower3, jnp.concatenate([one, rest, left.astype(BF16)], axis=0))
        return betas, run, run.T

    def block_terms(b, before_slab, midway):
        betas, run, across = small_terms(b)
        keys, decays, growths, lows, weighteds, ends = [], [], [], [], [], []
        sides = []
        for h in range(heads):
            k = unit(mixed(1, h, b))
            down = run[:, heads + h : heads + h + 1]
            along = across[heads + h : heads + h + 1, :]
            beta = betas[:, h : h + 1]
            last = down[BLOCK - 1 : BLOCK, :]
            decay = jnp.where(within, jnp.exp(jnp.minimum(down - along, 0.0)), 0.0)
            key = split(k)
            gram = dot3(key, key, ((1,), (1,)))
            lows.append(jnp.where(before, beta * decay * gram, 0.0))
            keys.append(key)
            decays.append(decay)
            growth = jnp.exp(down)
            growths.append(growth)
            ends.append(jnp.exp(last))
            weighteds.append((jnp.exp(last - down) * k).T)
        inverses = bases(lows)
        for h in range(heads):
            beta = betas[:, h : h + 1]
            v = mixed(2, h, b)
            scale = beta * growths[h]
            if before_slab is None:
                k = keys[h][0].astype(F32) + keys[h][1].astype(F32)
                sides.append(jnp.concatenate([-scale * k, beta * v], axis=1))
            else:
                moved = -scale * dot3(keys[h], before_slab[h])
                sides.append(
                    jnp.concatenate([moved[:, :dim], moved[:, dim:] + beta * v], axis=1)
                )
        span = BASE
        while 4 * span < BLOCK:
            area = (row // (4 * span) == col // (4 * span)) & (row // span > col // span)
            shares = [split(inv) for inv in inverses]
            links = [
                split(dot3(share, jnp.where(area, low, 0.0))) for share, low in zip(shares, lows)
            ]
            nexts = []
            for inv, share, link in zip(inverses, shares, links):
                pair = dot3(link, tuple(
                    jnp.concatenate([a, c], axis=1) for a, c in zip(share, link)
                ))
                nexts.append((inv - pair[:, :BLOCK], pair[:, BLOCK:]))
            inverses = [z + dot3(square, z) for z, square in nexts]
            span *= 4
        midway()
        area = row // span > col // span
        wide = [
            dot3(inv, jnp.concatenate([jnp.where(area, low, 0.0), side], axis=1))
            for inv, low, side in zip(inverses, lows, sides)
        ]
        links = [split(got[:, :BLOCK]) for got in wide]
        solved = [got[:, BLOCK:] for got in wide]
        level = span
        while level < BLOCK:
            nexts = []
            for link, have in zip(links, solved):
                share = split(have)
                more = level * 2 < BLOCK
                right = tuple(
                    jnp.concatenate([a, c], axis=1) for a, c in zip(share, link)
                ) if more else share
                got = dot3(link, right)
                nexts.append((got[:, : 2 * dim], got[:, 2 * dim :] if more else None))
            sign = -1.0 if level == span else 1.0
            solved = [have + sign * got for have, (got, _) in zip(solved, nexts)]
            links = [split(square) if square is not None else None for _, square in nexts]
            level *= 2
        slabs = []
        shares = [split(have) for have in solved]
        for h in range(heads):
            got = dot3(weighteds[h], shares[h])
            if before_slab is None:
                slabs.append(jnp.concatenate([ends[h] * eye + got[:, :dim], got[:, dim:]], axis=1))
            else:
                high, rest = before_slab[h]
                have = high.astype(F32) + rest.astype(F32)
                slabs.append(ends[h] * have + got)

        def outputs():
            for h in range(heads):
                q = unit(mixed(0, h, b))
                mix = decays[h] * dot3(q, keys[h], ((1,), (1,)))
                lead = growths[h] * q
                if before_slab is None:
                    got = dot3(mix, shares[h])
                    read, here = got[:, :dim] + lead, got[:, dim:]
                else:
                    right = tuple(
                        jnp.concatenate([a, c], axis=0)
                        for a, c in zip(shares[h], before_slab[h])
                    )
                    got = dot3(jnp.concatenate([mix, lead], axis=1), right)
                    read, here = got[:, :dim], got[:, dim:]
                reader[h, b] = read.astype(BF16)
                local[h, b] = here

        return slabs, outputs

    def columns_of(m):
        return pl.ds(pl.multiple_of((me ^ m) * columns, LANES), columns)

    own = pltpu.make_async_copy(w_ref.at[:, columns_of(0)], w_buf.at[0], own_sem)
    share = width // 2

    def part_of(which):
        return pl.ds(pl.multiple_of(which * share, share), share)

    moves, passes = {}, {}
    for m in range(1, n):
        if m in near:
            source, target = w_ref.at[:, columns_of(m)], w_buf.at[m]
        else:
            source, target = w_ref.at[part_of(odd), columns_of(m)], w_buf.at[m, part_of(odd)]
            passes[m] = remote(
                w_buf.at[m, part_of(odd)], w_buf.at[m, part_of(odd)], v_send, v_recv, (mate, me)
            )
        moves[m] = remote(
            source, target, w_send, w_recv.at[0 if m in near else 1], (seq, me ^ m)
        )
    half_slots = w_buf.at[pl.ds(0, len(passes) // 2)]
    all_halves = remote(half_slots, half_slots, v_send, v_recv, (mate, me))
    far_halves = remote(half_slots, half_slots, w_send, w_recv.at[1], (seq, me ^ n // 2))
    all_slots = w_buf.at[pl.ds(0, len(passes) // 2 + len(near))]
    all_moves = remote(all_slots, all_slots, w_send, w_recv.at[0], (seq, me ^ 1))

    def arrive_block(b):
        for m in far:
            if low_bit(m) > 1:
                arrive(m, b)

    direct = [m for m in far if low_bit(m) > 1]
    passed = [m for m in far if low_bit(m) == 1]
    slabs = None
    outputs = []
    add_prior()
    arrive_block(0)
    add(direct, 0, BLOCK, first_cols)
    for b in range(blocks):
        for m in passed:
            arrive(m, b)
        add(passed, b * BLOCK, BLOCK, first_cols)

        def midway():
            if b + 1 < blocks:
                arrive_block(b + 1)
                add(direct, (b + 1) * BLOCK, BLOCK, first_cols)
            if b + 2 == max(blocks, 2):
                own.start()
                for m in far + near:
                    moves[m].start()

        prior_slab = None if slabs is None else [split(value) for value in slabs]
        slabs, later = block_terms(b, prior_slab, midway)
        outputs.append(later)

    swaps_a, swaps_c = [], []
    for h in range(heads):
        slab_c[h] = slabs[h][:, dim:].astype(slab_c.dtype)
        slab_a[h] = slabs[h][:, :dim].astype(slab_a.dtype)
        swaps_a.append(
            remote(slab_a.at[h], mate_a.at[h], sa_send.at[h], sa_recv.at[h], (mate, me))
        )
        swaps_c.append(
            remote(slab_c.at[h], mate_c.at[h], sc_send.at[h], sc_recv.at[h], (mate, me))
        )
    for h in range(heads):

        @pl.when(gives_c[h])
        def _():
            swaps_c[h].start()

        @pl.when(gives_a[h])
        def _():
            swaps_a[h].start()

    blank = jnp.zeros((dim, dim), slab_a.dtype)
    for h in range(heads):

        @pl.when(jnp.logical_not(takes_a[h]))
        def _():
            mate_a[h] = blank

        @pl.when(jnp.logical_not(takes_c[h]))
        def _():
            mate_c[h] = blank
        pre_c[h] = jnp.zeros((dim, dim), F32)

    for at in range(0, tokens, step):
        add(far, at, step, rest_cols)
    for h in range(heads):
        place = pl.ds(PRIOR, tokens), pl.ds(g_at + h * dim, dim)
        gate = raw[place]
        raw[place] = gain[...] * (gate * jax.nn.sigmoid(gate))
    for later in outputs:
        later()

    def total_copy(source, target, send_sem, recv_sem, r, h, j):
        return remote(
            source.at[r, h], target.at[r, h], send_sem.at[rounds[r] // 2 - 1 + j, h],
            recv_sem.at[r, h], (seq + 2 + 2 * j, me),
        )

    totals_c, totals_a = {}, {}
    for r, half in enumerate(rounds):
        for h in range(heads):
            for j in range(half // 2):
                totals_c[r, h, j] = total_copy(go_c, in_c, c_send, c_recv, r, h, j)
                if r + 1 < len(rounds):
                    totals_a[r, h, j] = total_copy(go_a, in_a, a_send, a_recv, r, h, j)
    asides = {
        h: remote(go_c.at[0, h], in_c.at[0, h], side_send.at[h - lone], c_recv.at[0, h], (seq + 1, me))
        for h in range(lone, heads) if rounds
    }
    pair_a, pair_c, firsts = [], [], []

    def giver(r, h):
        return sources[r] & (seq != 0) if r == 0 and h >= lone else sources[r]

    def send_total(r, h):
        @pl.when(giver(r, h))
        def _():
            total = pair_c[h] if r == 0 else dot(pair_a[h], pre_c[h]) + pair_c[h]
            go_c[r, h] = total.astype(go_c.dtype)
            for j in reversed(range(rounds[r] // 2)):
                totals_c[r, h, j].start()

            if r + 1 == len(rounds):
                return

            @pl.when(whole[r])
            def _():
                total = pair_a[h] if r == 0 else dot(pair_a[h], pre_a[h])
                go_a[r, h] = total.astype(go_a.dtype)
                for j in reversed(range(rounds[r] // 2)):
                    totals_a[r, h, j].start()

        if r == 0 and h in asides:

            @pl.when(starts)
            def _():
                asides[h].start()

    def take_total(r, h):
        first = seq % rounds[r] < 2

        @pl.when(uppers[r])
        def _():
            totals_c[r, h, 0].wait_recv()

            @pl.when(first)
            def _():
                pre_c[h] = in_c[r, h].astype(F32)

            @pl.when(jnp.logical_not(first))
            def _():
                pre_c[h] = dot(pre_a[h], in_c[r, h]) + pre_c[h]

            if r + 1 == len(rounds):
                return

            @pl.when(whole[r])
            def _():
                totals_a[r, h, 0].wait_recv()

                @pl.when(first)
                def _():
                    pre_a[h] = in_a[r, h].astype(F32)

                @pl.when(jnp.logical_not(first))
                def _():
                    pre_a[h] = dot(pre_a[h], in_a[r, h])

    def hand_over():
        far_halves.wait_recv()
        for m in passes:
            passes[m].start()

    lifts = {}

    def lift_slot(m, h, b):
        if m in forwards:
            return (forwards.index(m) * blocks + b) * heads + h
        return (len(forwards) * heads + lasts.index(m)) * blocks + b

    def lift(m, bit, h, b):
        got = m | bit
        return remote(
            hid.at[m, b, h], hid.at[got, b, h],
            h_send.at[got - 1], h_recv.at[lift_slot(got, h, b)], (seq, me ^ bit),
        )

    def forward(m, h, b):
        limit = n if m == 0 else low_bit(m)
        for bit in bits:
            if bit < limit:
                lifts[m | bit, h, b] = lift(m, bit, h, b)
                lifts[m | bit, h, b].start()

    states = []

    def read(h, b):
        head_out = dot(reader[h, b], states[h]) + local[h, b]
        gate = raw[pl.ds(PRIOR + b * BLOCK, BLOCK), pl.ds(g_at + h * dim, dim)]
        scaled = head_out * lax.rsqrt(
            jnp.mean(head_out * head_out, axis=-1, keepdims=True) + norm_floor
        )
        hid[0, b, h] = (scaled * gate).astype(BF16)
        forward(0, h, b)

    upper = uppers[-1] if rounds else seq < 0

    def relay(h):
        for r in range(len(rounds) - 1):
            take_total(r, h)
            send_total(r + 1, h)

    for h in range(heads):
        @pl.when(takes_c[h])
        def _():
            swaps_c[h].wait_recv()

        @pl.when(takes_a[h])
        def _():
            swaps_a[h].wait_recv()

        here_a, here_c = slab_a[h].astype(F32), slab_c[h].astype(F32)
        there_a, there_c = mate_a[h].astype(F32), mate_c[h].astype(F32)
        left = jnp.where(is_odd, here_a, there_a)
        right_a = jnp.where(is_odd, there_a, here_a)
        right_c = jnp.where(is_odd, there_c, here_c)
        back_c = jnp.where(is_odd, here_c, there_c)
        moved = dot(left, jnp.concatenate([right_a, right_c], axis=1))
        pair_a.append(moved[:, :dim])
        pair_c.append(moved[:, dim:] + back_c)
        firsts.append((right_a, right_c))
        if rounds:
            send_total(0, h)

        @pl.when(jnp.logical_not(upper))
        def _():
            relay(h)


    hand_over()

    for h in range(heads):
        @pl.when(upper)
        def _():
            relay(h)

        if rounds:
            take_total(len(rounds) - 1, h)
        first_a, first_c = firsts[h]
        state = pre_c[h]
        states.append(jnp.where(is_odd, dot(first_a, state) + first_c, state))
        for b in range(blocks):
            read(h, b)

    own.wait()
    for m in near:
        moves[m].wait_recv()

    def rows_of(m, b):
        return jnp.concatenate([hid[m, b, h] for h in range(heads)], axis=1)

    def settle(m, b):
        here = hid.at[m, b]
        remote(
            here, here, h_send.at[m - 1], h_recv.at[lift_slot(m, 0, b)], (seq, me ^ 1)
        ).wait_recv()

    for h in range(heads):
        for b in range(blocks):
            for m in forwards:
                lifts[m, h, b].wait_recv()
                forward(m, h, b)
            if h + 1 == heads:
                total = jnp.dot(rows_of(0, b), w_buf[0], preferred_element_type=F32)
                for m in near:
                    settle(m, b)
                    total = total + jnp.dot(rows_of(m, b), w_buf[m], preferred_element_type=F32)
                acc[b] = total
    all_halves.wait_recv()
    for b in range(blocks):
        total = acc[b]
        for m in far:
            if m in lasts:
                settle(m, b)
            total = total + jnp.dot(rows_of(m, b), w_buf[m], preferred_element_type=F32)
        out_ref[pl.ds(b * BLOCK, BLOCK), :] = total.astype(BF16)

    for m in range(1, n):
        remote(buf.at[m], buf.at[m], x_send.at[m - 1], x_recv.at[0], (seq, me ^ 1)).wait_send()
        remote(hid.at[m], hid.at[m], h_send.at[m - 1], h_recv.at[0], (seq, me ^ 1)).wait_send()
    for crossing in crossings:
        crossing.wait_send()
    all_moves.wait_send()
    all_halves.wait_send()

    for h in range(heads):

        @pl.when(gives_c[h])
        def _():
            swaps_c[h].wait_send()

        @pl.when(gives_a[h])
        def _():
            swaps_a[h].wait_send()

        if h in asides:

            @pl.when(starts)
            def _():
                asides[h].wait_send()

        for r, half in enumerate(rounds):

            @pl.when(giver(r, h))
            def _():
                for j in range(half // 2):
                    totals_c[r, h, j].wait_send()

                if r + 1 == len(rounds):
                    return

                @pl.when(whole[r])
                def _():
                    for j in range(half // 2):
                        totals_a[r, h, j].wait_send()

    @pl.when(has_next)
    def _():
        remote(prior, prior, p_send, p_recv, (seq + 1, me)).wait_send()


def on_device(
    seqs, n,
    layer_in, query_weight, key_weight, value_weight, gate_weight, beta_weight, decay_weight,
    conv_weight, decay_log, beta_bias, decay_bias, norm_gain, out_weight,
):
    tokens, feats = layer_in.shape
    model, width = query_weight.shape
    heads = beta_weight.shape[1]
    dim = width // heads
    blocks = tokens // BLOCK
    per_block = BLOCK // PIECE
    ways = (n // 2 - 1) * blocks
    total_width = 4 * width + LANES
    columns = out_weight.shape[1] // n
    vmem = pl.BlockSpec(memory_space=pltpu.VMEM)
    anywhere = pl.BlockSpec(memory_space=pl.ANY)
    dma = pltpu.SemaphoreType.DMA
    wire = BF16 if seqs <= 8 else F32
    steps = max(1, len(rounds_of(seqs)))
    most = max(1, seqs // 4)
    square = pltpu.VMEM((heads, dim, dim), wire)
    stage = pltpu.VMEM((steps, heads, dim, dim), wire)
    total = pltpu.VMEM((heads, dim, dim), F32)
    return pl.pallas_call(
        functools.partial(layer_kernel, seqs, n, heads),
        out_shape=pltpu.VMEM((tokens, columns), BF16),
        in_specs=[anywhere] * 13,
        out_specs=vmem,
        scratch_shapes=[
            pltpu.VMEM((model, total_width), BF16),
            pltpu.VMEM((LANES, model), F32),
            pltpu.VMEM((LANES, (BASE - 1) * LANES), BF16),
            pltpu.VMEM((tokens, feats), BF16),
            pltpu.VMEM((n, tokens, feats), BF16),
            pltpu.VMEM((n // 2 - 1, PRIOR, feats), BF16),
            pltpu.VMEM((n, PRIOR, feats), BF16),
            pltpu.VMEM((PRIOR + tokens, total_width), F32),
            pltpu.VMEM((heads, blocks, BLOCK, dim), F32),
            pltpu.VMEM((heads, blocks, BLOCK, dim), BF16),
            square, square, square, square,
            stage, stage, stage, stage,
            total, total,
            pltpu.VMEM((n, width, columns), BF16),
            pltpu.VMEM((n, blocks, heads, BLOCK, dim), BF16),
            pltpu.VMEM((blocks, BLOCK, columns), F32),
            pltpu.VMEM((heads, model), BF16),
            pltpu.VMEM((heads, model), BF16),
            pltpu.VMEM((conv_weight.shape[1], conv_weight.shape[0], width), F32),
            pltpu.VMEM((1, dim), F32),
            pltpu.SMEM((heads,), F32),
            pltpu.SMEM((heads,), F32),
            pltpu.SMEM((heads,), F32),
            dma(()),
            dma((7,)),
            dma(()),
            dma((n // 2 - 1,)),
            dma((n // 2 - 1,)),
            dma((n - 1,)),
            dma((ways * per_block + n // 2 * blocks,)),
            dma(()),
            dma(()),
            dma(()),
            dma(()),
            dma((2,)),
            dma(()),
            dma(()),
            dma((heads,)),
            dma((heads,)),
            dma((heads,)),
            dma((heads,)),
            dma((heads - heads // 2,)),
            dma((max(1, seqs // 4 - 1), heads)),
            dma((max(1, steps - 1), heads)),
            dma((max(1, seqs // 2 - 1), heads)),
            dma((steps, heads)),
            dma((n - 1,)),
            dma((ways * heads + n // 2 * blocks,)),
        ],
        compiler_params=pltpu.CompilerParams(
            collective_id=0, has_side_effects=True, vmem_limit_bytes=60 * 1024 * 1024
        ),
    )(
        layer_in, query_weight, key_weight, value_weight, gate_weight,
        beta_weight.T, decay_weight.T, conv_weight.transpose(1, 0, 2),
        decay_log, beta_bias, decay_bias, norm_gain[None], out_weight,
    )


def solution(mesh):
    return jax.shard_map(
        functools.partial(on_device, mesh.shape["seq"], mesh.shape["head"]),
        mesh=mesh,
        in_specs=(
            P("seq", "head"),
            P(None, "head"),
            P(None, "head"),
            P(None, "head"),
            P(None, "head"),
            P(None, "head"),
            P(None, "head"),
            P(None, None, "head"),
            P("head"),
            P("head"),
            P("head"),
            P(),
            P("head", None),
        ),
        out_specs=P("seq", "head"),
        check_vma=False,
    )
```
